32 devices in a mesh: gx: 8 (over z, y), gy: 4 (over x, core).
Axes of the slice: x: 2, y: 2, z: 4, core: 2. Of those that a mesh axis runs over, the one named last changes fastest.
Arguments:
- rhs: bfloat16 [512, 32768], P(None, ('gy', 'gx')), may hold values from -6 to 6
- leaf_inverse: bfloat16 [32, 1024, 1024], P(('gy', 'gx')), may hold values from -0.1875 to 0.1875
- up_basis: bfloat16 [5, 128, 32768], P(None, None, ('gy', 'gx')), may hold values from -0.25 to 0.25
- projection: bfloat16 [5, 256, 32768], P(None, None, ('gy', 'gx')), may hold values from -0.13258252 to 0.13258252, as said below
Outputs:
- solution: float32 [512, 32768], P(None, ('gy', 'gx'))
The draws below stay inside these ranges and needn't reach their ends.
Inputs may be any that keep to these rules, and one draw needn't show every extreme that they name: `projection`: rows of level h (counted from 1) have entries of order (2^h * 1024)^(-1/2).
All inputs are finite; a program needn't handle non-finite values.
Results may differ from the reference program's by a relative error of at most 0.0095.
Values sent between devices are 32-bit elements; how exact they have to be, the bound alone decides.
A program may use at most 64 MiB of HBM per device.

```python
import jax
import jax.numpy as jnp
from jax import lax

LEAF = 1024
RANK = 128
RHS = 512
LEVELS = 5
POINTS = 32768


def draw_projection(key, part):
    heights = jnp.arange(1, LEVELS + 1).astype(jnp.float32)
    scales = 1.0 / jnp.sqrt(LEAF * 2.0 ** heights)
    values = jnp.clip(jax.random.normal(key, (LEVELS, 2 * RANK, POINTS), jnp.float32), -6.0, 6.0)
    return (values * scales[:, None, None]).astype(jnp.bfloat16)


def shard_levels(rng, shape, pieces, least, high):
    level, own = 1.0, jax.random.fold_in(rng, 6)
    for position, shards_of in pieces:
        draws = jnp.exp(jax.random.uniform(jax.random.fold_in(own, position), (shards_of,), jnp.float32, least / len(pieces), high / len(pieces)))
        level = level * jnp.repeat(draws, shape[position] // shards_of).reshape([-1 if axis == position else 1 for axis in range(len(shape))])
    return level


def gaussian(key, dims, deviation, limit, shards=(), dtype=jnp.bfloat16):
    factor_of = shard_levels(key, dims, shards, -0.22, 0.18) if shards else 1.0
    array = jax.random.normal(key, dims, jnp.float32) * deviation * factor_of
    return jnp.minimum(jnp.maximum(array, -limit), limit).astype(dtype)


def setup_inputs(seed: int = 0) -> dict:
    arg_keys = jax.random.split(jax.random.key(seed), 5)
    return {
        "rhs": gaussian(arg_keys[0], (RHS, POINTS), 1.0, 6.0, ((1, 32),)),
        "leaf_inverse": gaussian(arg_keys[1], (POINTS // LEAF, LEAF, LEAF), LEAF ** -0.5, 0.1875, ((0, 32),)),
        "up_basis": gaussian(arg_keys[2], (LEVELS, RANK, POINTS), (4 * RANK) ** -0.5, 0.25, ((2, 32),)),
        "projection": draw_projection(jax.random.fold_in(arg_keys[4], 71), 0),
    }


def leaf_apply(operands):
    return jnp.dot(operands[0], operands[1], preferred_element_type=jnp.float32)


def project_leaf(operands):
    return lax.dot_general(operands[0], operands[1], (((1,), (1,)), ((), ())), preferred_element_type=jnp.float32)


def reference(rhs, leaf_inverse, up_basis, projection):
    leaves = leaf_inverse.shape[0]
    blocks = rhs.reshape(RHS, leaves, LEAF).transpose(1, 0, 2)
    state = lax.map(leaf_apply, (blocks, leaf_inverse))
    for height in range(1, LEVELS + 1):
        rounded = state.astype(jnp.bfloat16)
        basis_rows = projection[height - 1].reshape(2 * RANK, leaves, LEAF).transpose(1, 0, 2)
        up_rows = up_basis[height - 1].reshape(RANK, leaves, LEAF).transpose(1, 0, 2)
        partial_value = lax.map(project_leaf, (rounded, basis_rows))
        groups = leaves // (2 ** height)
        node_total = partial_value.reshape(groups, 2 ** height, RHS, 2, RANK).sum(axis=1)
        node_total = jnp.moveaxis(node_total, 2, 1)
        half_count = 2 ** (height - 1)
        coefficient = jnp.broadcast_to(node_total[:, :, None], (groups, 2, half_count, RHS, RANK))
        coefficient = coefficient.reshape(leaves, RHS, RANK).astype(jnp.bfloat16)
        state = state - lax.map(leaf_apply, (coefficient, up_rows))
    return state.transpose(1, 0, 2).reshape(RHS, leaves * LEAF)
```

```python
import functools

import jax
import jax.numpy as jnp
from jax import lax
from jax.experimental import pallas as pl
from jax.experimental.pallas import tpu as pltpu
from jax.sharding import PartitionSpec as P

CHUNKS = 2
SUBLANES = 8
F32 = jnp.float32
BF16 = jnp.bfloat16
MESH = pl.DeviceIdType.MESH


def level_plan(height, bits_x, rows):
    top = height - 1
    groups = []
    low = [b for b in range(min(top, bits_x))]
    high = [b for b in range(bits_x, top)]
    if top == bits_x:
        groups.append([top])
    elif top > bits_x:
        groups.append([bits_x])
        last = [top] + high[1:]
        if len(low) <= 3 and rows >> len(low) + len(high) >= SUBLANES:
            last, low = last + low, []
        groups.append(last)
    if top < bits_x and len(low) < 3:
        groups.append(low + [top])
    else:
        while low:
            groups.append(low[:3])
            low = low[3:]
        if top < bits_x:
            groups.append([top])
    phases = []
    for bits in groups:
        split = [b for b in bits if b != top]
        if rows >> len(split) < SUBLANES:
            assert top not in bits
            phases.append((bits, []))
        else:
            rows >>= len(split)
            phases.append((bits, split))
    return phases


def masks_of(bits):
    masks = [0]
    for b in bits:
        masks += [m | 1 << b for m in masks]
    return masks[1:]


def triples(bits):
    return [bits[i : i + 3] for i in range(0, len(bits), 3)]


def sub_index(pos, bits):
    index = 0
    for k, b in enumerate(bits):
        index = index + ((pos >> b) & 1) * (1 << k)
    return index


class Step:
    def __init__(self, kind, bits, half, block, split, src, landing, dst, shape, sem):
        self.kind, self.masks = kind, masks_of(bits)
        self.half, self.block, self.split = half, block, split
        self.src, self.landing, self.dst = src, landing, dst
        self.shape, self.sem = shape, sem


class Buffers:
    def __init__(self):
        self.shapes, self.sems = [], 0

    def new(self, *shape):
        self.shapes.append(shape)
        return len(self.shapes) - 1

    def reduce(self, src, shape, bits, half=None, block=None, split=()):
        c, b, n, r = shape
        shape = (1 if half is not None else c, 1 if block is not None else b, n >> len(split), r)
        landing = self.new(2 ** len(bits) - 1, *shape)
        step = Step("reduce", bits, half, block, list(split), src, landing, self.new(*shape), shape, self.sems)
        self.sems += len(step.masks)
        return step

    def gather(self, src, shape, split, block=None):
        c, b, n, r = shape
        bits = list(split) + ([] if block is None else [block])
        whole = (c, b if block is None else 2, n << len(split), r)
        step = Step("gather", bits, None, block, list(split), src, None, self.new(*whole), shape, self.sems)
        self.sems += len(step.masks)
        return step

    def chain(self, src, shape, makers):
        steps = []
        for make in makers:
            steps.append(make(src, shape))
            src, shape = steps[-1].dst, self.shapes[steps[-1].dst]
        return steps, src, shape


def group_levels(levels, rows):
    groups, height = [], 1
    while height <= levels:
        pair = height % 2 == 0 and height < levels and rows // 2 >> height - 1 >= SUBLANES
        groups.append((height, height + 1) if pair else (height,))
        height += len(groups[-1])
    return groups


def build_plan(levels, bits_x, rows, rank):
    plan, space, tables = [], Buffers(), {}
    for group in group_levels(levels, rows):
        height = group[0]
        top = height - 1
        entry = {"group": group}
        if len(group) == 1:
            shape = (2, 1, rows, rank)
            tables[height] = space.new(*shape)
            makers, splits = [], []
            for bits, split in level_plan(height, bits_x, rows):
                half = top if top in bits else None
                makers.append(functools.partial(space.reduce, bits=bits, half=half, split=split))
                if split:
                    splits.append(split)
            entry["reduce"], src, shape = space.chain(tables[height], shape, makers)
            makers = [functools.partial(space.gather, split=s) for s in reversed(splits)]
            entry["gather"], entry["result"], _ = space.chain(src, shape, makers)
        else:
            low = list(range(top))
            shape = (2, 2, rows // 2, rank)
            first, second = space.new(*shape), space.new(*shape)
            tables[height], tables[height + 1] = first, second
            parts = [functools.partial(space.reduce, bits=g, split=g) for g in triples(low)]
            own = functools.partial(space.reduce, bits=[top], half=top)
            entry["early"] = top == bits_x
            if entry["early"]:
                one = [own] + parts
                two = [functools.partial(space.reduce, bits=[top], block=top)] + parts
            elif len(low) < 3:
                one = [functools.partial(space.reduce, bits=low + [top], half=top, split=low)]
                two = parts
            else:
                one, two = parts + [own], parts
            entry["one"], src, shape = space.chain(first, shape, one)
            entry["owned"], n = src, shape[2]
            makers = [functools.partial(space.gather, split=g) for g in reversed(triples(low))]
            entry["gather_one"], entry["result_one"], _ = space.chain(src, shape, makers)
            entry["two"], entry["partial"], _ = space.chain(second, (2, 2, rows // 2, rank), two)
            shape = (2, 2, n, rank)
            entry["joined"] = space.new(*shape)
            entry["last"] = space.reduce(entry["joined"], shape, [top, height], half=height, block=top)
            shape = entry["last"].shape
            if len(low) <= 3:
                makers = [functools.partial(space.gather, split=low, block=top)]
            else:
                makers = [functools.partial(space.gather, split=[], block=top)]
                makers += [functools.partial(space.gather, split=g) for g in reversed(triples(low))]
            entry["gather_two"], entry["result_two"], _ = space.chain(entry["last"].dst, shape, makers)
        plan.append(entry)
    return plan, space, tables


def build_sums(plan, rank):
    space, sums = Buffers(), []
    for entry in plan:
        if len(entry["group"]) == 1:
            continue
        height = entry["group"][0]
        low = list(range(height - 1))
        shape = (2, 1, rank, rank)
        src = space.new(*shape)
        makers, splits, n = [], [], rank
        for g in triples(low):
            split = g if len(low) > 1 and n >> len(g) >= SUBLANES else []
            n >>= len(split)
            makers.append(functools.partial(space.reduce, bits=g, split=split))
            if split:
                splits.append(split)
        steps, dst, shape = space.chain(src, shape, makers)
        makers = [functools.partial(space.gather, split=s) for s in reversed(splits)]
        more, dst, _ = space.chain(dst, shape, makers)
        sums.append((height, src, steps + more, dst))
    return sums, space


def kernel(dims, plan, tables, sums, counts, rhs_hbm, leaf_hbm, up_hbm, proj_hbm, state, last_ref, *scratch):
    bits_x, bits_y, levels, chunks, rows, rank = dims
    rhs, leaf, up, proj, rounded, coef, mix, mix_sum = scratch[:8]
    in_sems, send_sems, recv_sems, sum_send, sum_recv = scratch[8:13]
    per_chunk = counts[0]
    gx, gy = lax.axis_index("gx"), lax.axis_index("gy")
    pos = gy * (1 << bits_x) + gx

    def device(mask):
        return {"gx": gx ^ (mask & ((1 << bits_x) - 1)), "gy": gy ^ (mask >> bits_x)}

    loads = {
        "rhs": pltpu.make_async_copy(rhs_hbm, rhs, in_sems.at[0]),
        "leaf": pltpu.make_async_copy(leaf_hbm.at[0], leaf, in_sems.at[1]),
    }
    for level in range(levels):
        loads["proj", level] = pltpu.make_async_copy(proj_hbm.at[level], proj.at[level], in_sems.at[2 + 2 * level])
        if level < levels - 1:
            loads["up", level] = pltpu.make_async_copy(up_hbm.at[level], up.at[level], in_sems.at[3 + 2 * level])
    for load in loads.values():
        load.start()

    def need(*key):
        load = loads.pop(key if len(key) > 1 else key[0], None)
        if load is not None:
            load.wait()

    greeted = {1 << b for b in range(bits_x + bits_y)}
    for entry in plan:
        group = entry["group"]
        if len(group) == 1:
            for step in entry["reduce"] + entry["gather"]:
                greeted.update(step.masks)
        elif group[0] == bits_x + 1:
            greeted.update(entry["last"].masks)
        else:
            for step in entry["one"]:
                greeted.update(step.masks)
    barrier = pltpu.get_barrier_semaphore()
    for mask in sorted(greeted):
        pl.semaphore_signal(barrier, inc=1, device_id=device(mask), device_id_type=MESH)

    sent = []

    def start(step, bufs, send, recv):
        src, dst = bufs[step.src], bufs[step.dst]
        n = step.shape[2]

        def piece(who):
            halves = pl.ds(0, step.shape[0]) if step.half is None else pl.ds((who >> step.half) & 1, 1)
            blocks = pl.ds(0, step.shape[1]) if step.block is None else pl.ds((who >> step.block) & 1, 1)
            return halves, blocks, pl.ds(pl.multiple_of(sub_index(who, step.split) * n, n), n)

        copies = []
        for k, mask in enumerate(step.masks):
            if step.kind == "gather":
                frm, to = src, dst.at[piece(pos)]
            else:
                frm, to = src.at[piece(pos ^ mask)], bufs[step.landing].at[k]
            copy = pltpu.make_async_remote_copy(
                src_ref=frm,
                dst_ref=to,
                send_sem=send(step.sem + k),
                recv_sem=recv(step.sem + k),
                device_id=device(mask),
                device_id_type=MESH,
            )
            copy.start()
            copies.append(copy)
        sent.extend(copies)
        if step.kind == "gather":
            dst[piece(pos)] = src[...]

        def finish():
            for copy in copies:
                copy.wait_recv()
            if step.kind == "reduce":
                total = src[piece(pos)]
                for k in range(len(step.masks)):
                    total = total + bufs[step.landing][k]
                dst[...] = total

        return finish

    def mixing(low, high):
        return low * levels + high

    def flow(chunk):
        lo = chunk * rows
        bufs = scratch[13 + chunk * per_chunk : 13 + (chunk + 1) * per_chunk]
        span = slice(lo, lo + rows)

        def begin(step):
            return start(step, bufs, lambda k: send_sems.at[chunk, k], lambda k: recv_sems.at[chunk, k])

        def project(height):
            need("proj", height - 1)
            table = bufs[tables[height]]
            for half in range(2):
                value = lax.dot_general(
                    rounded[span, :],
                    proj[height - 1, half * rank : (half + 1) * rank, :],
                    (((1,), (1,)), ((), ())),
                    preferred_element_type=F32,
                )
                table[half] = value.reshape(table.shape[1:])

        def keep(height, ref):
            value = ref[0].reshape(rows, rank).astype(BF16)
            if height == levels:
                last_ref[span, :] = value
            else:
                coef[height - 1, span, :] = value

        def correct(done, heights):
            for height in heights:
                delta = jnp.dot(coef[done - 1, span, :], mix[mixing(done, height)], preferred_element_type=F32)
                table = bufs[tables[height]]
                for half in range(2):
                    part = delta[:, half * rank : (half + 1) * rank]
                    table[half] = table[half] - part.reshape(table.shape[1:])

        def update(heights):
            value = state[span, :]
            for height in heights:
                need("up", height - 1)
                value = value - jnp.dot(coef[height - 1, span, :], up[height - 1], preferred_element_type=F32)
            state[span, :] = value

        need("rhs")
        need("leaf")
        value = jnp.dot(rhs[span, :], leaf[...], preferred_element_type=F32)
        state[span, :] = value
        rounded[span, :] = value.astype(BF16)
        project(1)
        if chunk == 0:
            pl.semaphore_wait(barrier, len(greeted))

        later = []
        for index, entry in enumerate(plan):
            group = entry["group"]
            after = [h for e in plan[index + 1 : index + 2] for h in e["group"]]
            beyond = [h for e in plan[index + 2 :] for h in e["group"]]
            if len(group) == 1:
                height = group[0]
                for step in entry["reduce"] + entry["gather"]:
                    finish = begin(step)
                    for work in later:
                        work()
                    later = []
                    yield
                    if height == 1 and step is entry["reduce"][0]:
                        for other in range(2, levels + 1):
                            project(other)
                    finish()
                keep(height, bufs[entry["result"]])
                if height < levels:
                    correct(height, after)
                    later = [functools.partial(correct, height, beyond), functools.partial(update, [height])]
            else:
                height = group[0]
                one, two = entry["one"], entry["two"]
                first, second = begin(one[0]), begin(two[0])
                for work in later:
                    work()
                later = []
                for i in range(max(len(one), len(two))):
                    yield
                    if i < len(one):
                        first()
                        if i + 1 < len(one):
                            first = begin(one[i + 1])
                        else:
                            fetch = begin(entry["gather_one"][0])
                    if i < len(two):
                        second()
                        if i + 1 < len(two):
                            second = begin(two[i + 1])
                owned, joined, base = bufs[entry["owned"]], bufs[entry["joined"]], bufs[entry["partial"]]
                n = owned.shape[2]
                complete(height)
                table = mix_sum[[s[0] for s in sums].index(height)]
                delta = jnp.dot(owned[0].reshape(2 * n, rank).astype(BF16), table, preferred_element_type=F32)
                for half in range(2):
                    for block in range(2):
                        part = delta[block * n : (block + 1) * n, half * rank : (half + 1) * rank]
                        if entry["early"]:
                            mine = ((pos >> height - 1) & 1) == block
                            joined[half, block] = jnp.where(mine, base[half, 0], 0.0) - part
                        else:
                            joined[half, block] = base[half, block] - part
                finish = begin(entry["last"])
                yield
                finish()
                finish = begin(entry["gather_two"][0])
                fetch()
                for step in entry["gather_one"][1:]:
                    fetch = begin(step)
                    yield
                    fetch()
                keep(height, bufs[entry["result_one"]])
                correct(height, after)
                later = [functools.partial(correct, height, beyond)]
                if after:
                    later.append(functools.partial(correct, height + 1, beyond))
                    later.append(functools.partial(update, [height, height + 1]))
                else:
                    update([height])
                    later = []
                yield
                finish()
                for step in entry["gather_two"][1:]:
                    finish = begin(step)
                    yield
                    finish()
                keep(height + 1, bufs[entry["result_two"]])
                if after:
                    correct(height + 1, after)

    sum_bufs = scratch[13 + chunks * per_chunk :]
    running = {}

    def compute(low, high):
        need("up", low - 1)
        need("proj", high - 1)
        value = lax.dot_general(up[low - 1], proj[high - 1], (((1,), (1,)), ((), ())), preferred_element_type=F32)
        mix[mixing(low, high)] = value.astype(BF16)
        return value

    def advance(height):
        for k, (key, src, steps, dst) in enumerate(sums):
            if key != height:
                continue
            if height in running:
                at, finish = running[height]
                if finish is None:
                    return
                finish()
            else:
                at = -1
            at += 1
            if at < len(steps):
                begun = start(steps[at], sum_bufs, lambda i: sum_send.at[i], lambda i: sum_recv.at[i])
                running[height] = (at, begun)
            else:
                running[height] = (at, None)
                for half in range(2):
                    mix_sum[k, :, half * rank : (half + 1) * rank] = sum_bufs[dst][half, 0].astype(BF16)

    def complete(height):
        while running.get(height, (0, 0))[1] is not None:
            advance(height)

    def summing():
        for low in range(1, levels):
            for high in range(low + 1, levels + 1):
                value = compute(low, high)
                for height, src, _, _ in sums:
                    if (low, high) == (height, height + 1):
                        for half in range(2):
                            sum_bufs[src][half, 0] = value[:, half * rank : (half + 1) * rank]
        order = [entry[0] for entry in sums]
        for height in order:
            advance(height)
            yield
            advance(height)
            yield
            if height != order[0]:
                complete(height)

    flows = [flow(chunk) for chunk in range(chunks)] + [summing()]
    while flows:
        left = []
        for item in flows:
            try:
                next(item)
                left.append(item)
            except StopIteration:
                pass
        flows = left
    for copy in sent:
        copy.wait_send()
    for key in list(loads):
        loads.pop(key).wait()


def shards(rhs, leaf_inverse, up_basis, projection):
    bits_x = lax.axis_size("gx").bit_length() - 1
    bits_y = lax.axis_size("gy").bit_length() - 1
    levels, rank, points = up_basis.shape
    rows = rhs.shape[0] // CHUNKS
    plan, space, tables = build_plan(levels, bits_x, rows, rank)
    sums, more = build_sums(plan, rank)
    dims = (bits_x, bits_y, levels, CHUNKS, rows, rank)
    hbm_spec = pl.BlockSpec(memory_space=pltpu.MemorySpace.HBM)
    vmem_spec = pl.BlockSpec(memory_space=pltpu.VMEM)
    state, coefficient = pl.pallas_call(
        functools.partial(kernel, dims, plan, tables, sums, (len(space.shapes),)),
        out_shape=(
            jax.ShapeDtypeStruct((rhs.shape[0], points), F32),
            jax.ShapeDtypeStruct((rhs.shape[0], rank), BF16),
        ),
        in_specs=[hbm_spec] * 4,
        out_specs=(vmem_spec, vmem_spec),
        scratch_shapes=[
            pltpu.VMEM(rhs.shape, BF16),
            pltpu.VMEM(leaf_inverse.shape[1:], BF16),
            pltpu.VMEM(up_basis.shape, BF16),
            pltpu.VMEM(projection.shape, BF16),
            pltpu.VMEM((rhs.shape[0], points), BF16),
            pltpu.VMEM((levels - 1, rhs.shape[0], rank), BF16),
            pltpu.VMEM((levels * (levels + 1), rank, 2 * rank), BF16),
            pltpu.VMEM((max(len(sums), 1), rank, 2 * rank), BF16),
            pltpu.SemaphoreType.DMA((2 + 2 * levels,)),
            pltpu.SemaphoreType.DMA((CHUNKS, space.sems)),
            pltpu.SemaphoreType.DMA((CHUNKS, space.sems)),
            pltpu.SemaphoreType.DMA((max(more.sems, 1),)),
            pltpu.SemaphoreType.DMA((max(more.sems, 1),)),
        ]
        + [pltpu.VMEM(shape, F32) for _ in range(CHUNKS) for shape in space.shapes]
        + [pltpu.VMEM(shape, F32) for shape in more.shapes],
        compiler_params=pltpu.CompilerParams(
            collective_id=0, has_side_effects=True, vmem_limit_bytes=44 * 2**20
        ),
    )(*[pltpu.with_memory_space_constraint(x, pltpu.MemorySpace.HBM) for x in (rhs, leaf_inverse, up_basis, projection)])
    return state - jnp.dot(coefficient, up_basis[levels - 1], preferred_element_type=F32)


def solution(mesh):
    return jax.shard_map(
        shards,
        mesh=mesh,
        in_specs=(
            P(None, ("gy", "gx")),
            P(("gy", "gx"), None, None),
            P(None, None, ("gy", "gx")),
            P(None, None, ("gy", "gx")),
        ),
        out_specs=P(None, ("gy", "gx")),
        check_vma=False,
    )
```

```python
import functools

import jax
import jax.numpy as jnp
from jax import lax
from jax.experimental import pallas as pl
from jax.experimental.pallas import tpu as pltpu
from jax.sharding import PartitionSpec as P

CHUNKS = 2
SUBLANES = 8
F32 = jnp.float32
BF16 = jnp.bfloat16
MESH = pl.DeviceIdType.MESH


def level_plan(height, bits_x, rows):
    top = height - 1
    groups = []
    low = [b for b in range(min(top, bits_x))]
    high = [b for b in range(bits_x, top)]
    if top == bits_x:
        groups.append([top])
    elif top > bits_x:
        groups.append([bits_x])
        last = [top] + high[1:]
        if len(low) <= 3 and rows >> len(low) + len(high) >= SUBLANES:
            last, low = last + low, []
        groups.append(last)
    if top < bits_x and len(low) < 3:
        groups.append(low + [top])
    else:
        while low:
            groups.append(low[:3])
            low = low[3:]
        if top < bits_x:
            groups.append([top])
    phases = []
    for bits in groups:
        split = [b for b in bits if b != top]
        if rows >> len(split) < SUBLANES:
            assert top not in bits
            phases.append((bits, []))
        else:
            rows >>= len(split)
            phases.append((bits, split))
    return phases


def masks_of(bits):
    masks = [0]
    for b in bits:
        masks += [m | 1 << b for m in masks]
    return masks[1:]


def triples(bits):
    return [bits[i : i + 3] for i in range(0, len(bits), 3)]


def pairs(bits):
    return [bits[i : i + 2] for i in range(0, len(bits), 2)]


def sub_index(pos, bits):
    index = 0
    for k, b in enumerate(bits):
        index = index + ((pos >> b) & 1) * (1 << k)
    return index


class Step:
    def __init__(self, kind, bits, half, block, split, src, landing, dst, shape, sem):
        self.kind, self.masks = kind, masks_of(bits)
        self.half, self.block, self.split = half, block, split
        self.src, self.landing, self.dst = src, landing, dst
        self.shape, self.sem = shape, sem


class Buffers:
    def __init__(self):
        self.shapes, self.sems = [], 0

    def new(self, *shape):
        self.shapes.append(shape)
        return len(self.shapes) - 1

    def reduce(self, src, shape, bits, half=None, block=None, split=()):
        c, b, n, r = shape
        shape = (1 if half is not None else c, 1 if block is not None else b, n >> len(split), r)
        landing = self.new(2 ** len(bits) - 1, *shape)
        step = Step("reduce", bits, half, block, list(split), src, landing, self.new(*shape), shape, self.sems)
        self.sems += len(step.masks)
        return step

    def gather(self, src, shape, split, block=None):
        c, b, n, r = shape
        bits = list(split) + ([] if block is None else [block])
        whole = (c, b if block is None else 2, n << len(split), r)
        step = Step("gather", bits, None, block, list(split), src, None, self.new(*whole), shape, self.sems)
        self.sems += len(step.masks)
        return step

    def chain(self, src, shape, makers):
        steps = []
        for make in makers:
            steps.append(make(src, shape))
            src, shape = steps[-1].dst, self.shapes[steps[-1].dst]
        return steps, src, shape


def group_levels(levels, rows):
    groups, height = [], 1
    while height <= levels:
        pair = height % 2 == 0 and height < levels and rows // 2 >> height - 1 >= SUBLANES
        groups.append((height, height + 1) if pair else (height,))
        height += len(groups[-1])
    return groups


def build_plan(levels, bits_x, rows, rank):
    plan, space, tables = [], Buffers(), {}
    for group in group_levels(levels, rows):
        height = group[0]
        top = height - 1
        entry = {"group": group}
        if len(group) == 1:
            shape = (2, 1, rows, rank)
            tables[height] = space.new(*shape)
            makers, splits = [], []
            for bits, split in level_plan(height, bits_x, rows):
                half = top if top in bits else None
                makers.append(functools.partial(space.reduce, bits=bits, half=half, split=split))
                if split:
                    splits.append(split)
            entry["reduce"], src, shape = space.chain(tables[height], shape, makers)
            makers = [functools.partial(space.gather, split=s) for s in reversed(splits)]
            entry["gather"], entry["result"], _ = space.chain(src, shape, makers)
        else:
            low = list(range(top))
            shape = (2, 2, rows // 2, rank)
            first, second = space.new(*shape), space.new(*shape)
            tables[height], tables[height + 1] = first, second
            parts = [functools.partial(space.reduce, bits=g, split=g) for g in pairs(low)]
            own = functools.partial(space.reduce, bits=[top], half=top)
            entry["early"] = top == bits_x
            one, two = [own] + parts, parts
            if entry["early"]:
                two = [functools.partial(space.reduce, bits=[top], block=top)] + parts
            entry["one"], src, shape = space.chain(first, shape, one)
            entry["owned"], n = src, shape[2]
            makers = [functools.partial(space.gather, split=g) for g in reversed(pairs(low))]
            entry["gather_one"], entry["result_one"], _ = space.chain(src, shape, makers)
            entry["two"], entry["partial"], _ = space.chain(second, (2, 2, rows // 2, rank), two)
            shape = (2, 2, n, rank)
            entry["joined"] = space.new(*shape)
            entry["last"] = space.reduce(entry["joined"], shape, [top, height], half=height, block=top)
            shape = entry["last"].shape
            if entry["early"]:
                nested = [b for g in reversed(pairs(low)) for b in g]
                makers = [functools.partial(space.gather, split=g) for g in triples(nested)]
                makers += [functools.partial(space.gather, split=[], block=top)]
            elif len(low) < 3:
                makers = [functools.partial(space.gather, split=low, block=top)]
            else:
                makers = [functools.partial(space.gather, split=[], block=top)]
                makers += [functools.partial(space.gather, split=g) for g in reversed(pairs(low))]
            entry["gather_two"], entry["result_two"], _ = space.chain(entry["last"].dst, shape, makers)
        plan.append(entry)
    return plan, space, tables


def build_sums(plan, rank):
    space, sums = Buffers(), []
    for entry in plan:
        if len(entry["group"]) == 1:
            continue
        height = entry["group"][0]
        low = list(range(height - 1))
        shape = (2, 1, rank, rank)
        src = space.new(*shape)
        makers, splits = [], []
        for bit in low[1:]:
            makers.append(functools.partial(space.reduce, bits=[bit], split=[bit]))
            splits.append([bit])
        makers.append(functools.partial(space.reduce, bits=low[:1]))
        steps, dst, shape = space.chain(src, shape, makers)
        makers = [functools.partial(space.gather, split=s) for s in reversed(splits)]
        more, dst, _ = space.chain(dst, shape, makers)
        sums.append((height, src, steps + more, dst))
    return sums, space


def kernel(dims, plan, tables, sums, counts, rhs_hbm, leaf_hbm, up_hbm, proj_hbm, state, last_ref, *scratch):
    bits_x, bits_y, levels, chunks, rows, rank = dims
    rhs, leaf, up, proj, rounded, coef, mix, mix_sum = scratch[:8]
    in_sems, send_sems, recv_sems, sum_send, sum_recv = scratch[8:13]
    per_chunk = counts[0]
    gx, gy = lax.axis_index("gx"), lax.axis_index("gy")
    pos = gy * (1 << bits_x) + gx

    def device(mask):
        return {"gx": gx ^ (mask & ((1 << bits_x) - 1)), "gy": gy ^ (mask >> bits_x)}

    loads = {
        "rhs": pltpu.make_async_copy(rhs_hbm, rhs, in_sems.at[0]),
        "leaf": pltpu.make_async_copy(leaf_hbm.at[0], leaf, in_sems.at[1]),
    }
    for level in range(levels):
        loads["proj", level] = pltpu.make_async_copy(proj_hbm.at[level], proj.at[level], in_sems.at[2 + 2 * level])
        if level < levels - 1:
            loads["up", level] = pltpu.make_async_copy(up_hbm.at[level], up.at[level], in_sems.at[3 + 2 * level])
    for load in loads.values():
        load.start()

    def need(*key):
        load = loads.pop(key if len(key) > 1 else key[0], None)
        if load is not None:
            load.wait()

    greeted = {1 << b for b in range(bits_x + bits_y)}
    for entry in plan:
        group = entry["group"]
        if len(group) == 1:
            for step in entry["reduce"] + entry["gather"]:
                greeted.update(step.masks)
        elif entry["early"]:
            greeted.update(entry["last"].masks)
        else:
            for step in entry["one"]:
                greeted.update(step.masks)
    barrier = pltpu.get_barrier_semaphore()
    for mask in sorted(greeted):
        pl.semaphore_signal(barrier, inc=1, device_id=device(mask), device_id_type=MESH)

    sent = []

    def start(step, bufs, send, recv):
        src, dst = bufs[step.src], bufs[step.dst]
        n = step.shape[2]

        def piece(who):
            halves = pl.ds(0, step.shape[0]) if step.half is None else pl.ds((who >> step.half) & 1, 1)
            blocks = pl.ds(0, step.shape[1]) if step.block is None else pl.ds((who >> step.block) & 1, 1)
            return halves, blocks, pl.ds(pl.multiple_of(sub_index(who, step.split) * n, n), n)

        copies = []
        for k, mask in enumerate(step.masks):
            if step.kind == "gather":
                frm, to = src, dst.at[piece(pos)]
            else:
                frm, to = src.at[piece(pos ^ mask)], bufs[step.landing].at[k]
            copy = pltpu.make_async_remote_copy(
                src_ref=frm,
                dst_ref=to,
                send_sem=send(step.sem + k),
                recv_sem=recv(step.sem + k),
                device_id=device(mask),
                device_id_type=MESH,
            )
            copy.start()
            copies.append(copy)
        sent.extend(copies)
        if step.kind == "gather":
            dst[piece(pos)] = src[...]

        def finish():
            for copy in copies:
                copy.wait_recv()
            if step.kind == "reduce":
                total = src[piece(pos)]
                for k in range(len(step.masks)):
                    total = total + bufs[step.landing][k]
                dst[...] = total

        return finish

    def mixing(low, high):
        return low * levels + high

    def flow(chunk):
        lo = chunk * rows
        bufs = scratch[13 + chunk * per_chunk : 13 + (chunk + 1) * per_chunk]
        span = slice(lo, lo + rows)

        def begin(step):
            return start(step, bufs, lambda k: send_sems.at[chunk, k], lambda k: recv_sems.at[chunk, k])

        def project(height):
            need("proj", height - 1)
            table = bufs[tables[height]]
            for half in range(2):
                value = lax.dot_general(
                    rounded[span, :],
                    proj[height - 1, half * rank : (half + 1) * rank, :],
                    (((1,), (1,)), ((), ())),
                    preferred_element_type=F32,
                )
                table[half] = value.reshape(table.shape[1:])

        def keep(height, ref):
            value = ref[0].reshape(rows, rank).astype(BF16)
            if height == levels:
                last_ref[span, :] = value
            else:
                coef[height - 1, span, :] = value

        def correct(done, heights):
            for height in heights:
                delta = jnp.dot(coef[done - 1, span, :], mix[mixing(done, height)], preferred_element_type=F32)
                table = bufs[tables[height]]
                for half in range(2):
                    part = delta[:, half * rank : (half + 1) * rank]
                    table[half] = table[half] - part.reshape(table.shape[1:])

        def update(heights):
            value = state[span, :]
            for height in heights:
                need("up", height - 1)
                value = value - jnp.dot(coef[height - 1, span, :], up[height - 1], preferred_element_type=F32)
            state[span, :] = value

        need("rhs")
        need("leaf")
        value = jnp.dot(rhs[span, :], leaf[...], preferred_element_type=F32)
        state[span, :] = value
        rounded[span, :] = value.astype(BF16)
        project(1)
        if chunk == 0:
            pl.semaphore_wait(barrier, len(greeted))

        later = []
        for index, entry in enumerate(plan):
            group = entry["group"]
            after = [h for e in plan[index + 1 : index + 2] for h in e["group"]]
            beyond = [h for e in plan[index + 2 :] for h in e["group"]]
            if len(group) == 1:
                height = group[0]
                for step in entry["reduce"] + entry["gather"]:
                    finish = begin(step)
                    for work in later:
                        work()
                    later = []
                    yield
                    if height == 1 and step is entry["reduce"][0]:
                        for other in range(2, levels + 1):
                            project(other)
                    finish()
                keep(height, bufs[entry["result"]])
                if height < levels:
                    correct(height, after)
                    later = [functools.partial(correct, height, beyond), functools.partial(update, [height])]
            else:
                height = group[0]
                one, two = entry["one"], entry["two"]
                first, second = begin(one[0]), begin(two[0])
                for work in later:
                    work()
                later = []
                for i in range(max(len(one), len(two))):
                    yield
                    if i < len(one):
                        first()
                        if i + 1 < len(one):
                            first = begin(one[i + 1])
                        else:
                            fetch = begin(entry["gather_one"][0])
                    if i < len(two):
                        second()
                        if i + 1 < len(two):
                            second = begin(two[i + 1])
                owned, joined, base = bufs[entry["owned"]], bufs[entry["joined"]], bufs[entry["partial"]]
                n = owned.shape[2]
                complete(height)
                table = mix_sum[[s[0] for s in sums].index(height)]
                delta = jnp.dot(owned[0].reshape(2 * n, rank).astype(BF16), table, preferred_element_type=F32)
                for half in range(2):
                    for block in range(2):
                        part = delta[block * n : (block + 1) * n, half * rank : (half + 1) * rank]
                        if entry["early"]:
                            mine = ((pos >> height - 1) & 1) == block
                            joined[half, block] = jnp.where(mine, base[half, 0], 0.0) - part
                        else:
                            joined[half, block] = base[half, block] - part
                finish = begin(entry["last"])
                yield
                finish()
                finish = begin(entry["gather_two"][0])
                fetch()
                for step in entry["gather_one"][1:]:
                    fetch = begin(step)
                    yield
                    fetch()
                keep(height, bufs[entry["result_one"]])
                correct(height, after)
                later = [functools.partial(correct, height, beyond)]
                if after:
                    later.append(functools.partial(correct, height + 1, beyond))
                    later.append(functools.partial(update, [height, height + 1]))
                else:
                    update([height])
                    later = []
                yield
                finish()
                for step in entry["gather_two"][1:]:
                    finish = begin(step)
                    yield
                    finish()
                keep(height + 1, bufs[entry["result_two"]])
                if after:
                    correct(height + 1, after)

    sum_bufs = scratch[13 + chunks * per_chunk :]
    running = {}

    def compute(low, high):
        need("up", low - 1)
        need("proj", high - 1)
        value = lax.dot_general(up[low - 1], proj[high - 1], (((1,), (1,)), ((), ())), preferred_element_type=F32)
        mix[mixing(low, high)] = value.astype(BF16)
        return value

    def advance(height):
        for k, (key, src, steps, dst) in enumerate(sums):
            if key != height:
                continue
            if height in running:
                at, finish = running[height]
                if finish is None:
                    return
                finish()
            else:
                at = -1
            at += 1
            if at < len(steps):
                begun = start(steps[at], sum_bufs, lambda i: sum_send.at[i], lambda i: sum_recv.at[i])
                running[height] = (at, begun)
            else:
                running[height] = (at, None)
                for half in range(2):
                    mix_sum[k, :, half * rank : (half + 1) * rank] = sum_bufs[dst][half, 0].astype(BF16)

    def complete(height):
        while running.get(height, (0, 0))[1] is not None:
            advance(height)

    def summing():
        for low in range(1, levels):
            for high in range(low + 1, levels + 1):
                value = compute(low, high)
                for height, src, _, _ in sums:
                    if (low, high) == (height, height + 1):
                        for half in range(2):
                            sum_bufs[src][half, 0] = value[:, half * rank : (half + 1) * rank]
        for height, _, _, _ in sums[1:]:
            advance(height)
        yield
        for _ in range(max([0] + [len(steps) + 1 for _, _, steps, _ in sums])):
            for height, _, _, _ in sums:
                advance(height)
            yield

    flows = [flow(chunk) for chunk in range(chunks)] + [summing()]
    while flows:
        left = []
        for item in flows:
            try:
                next(item)
                left.append(item)
            except StopIteration:
                pass
        flows = left
    for copy in sent:
        copy.wait_send()
    for key in list(loads):
        loads.pop(key).wait()


def shards(rhs, leaf_inverse, up_basis, projection):
    bits_x = lax.axis_size("gx").bit_length() - 1
    bits_y = lax.axis_size("gy").bit_length() - 1
    levels, rank, points = up_basis.shape
    rows = rhs.shape[0] // CHUNKS
    plan, space, tables = build_plan(levels, bits_x, rows, rank)
    sums, more = build_sums(plan, rank)
    dims = (bits_x, bits_y, levels, CHUNKS, rows, rank)
    hbm_spec = pl.BlockSpec(memory_space=pltpu.MemorySpace.HBM)
    vmem_spec = pl.BlockSpec(memory_space=pltpu.VMEM)
    state, coefficient = pl.pallas_call(
        functools.partial(kernel, dims, plan, tables, sums, (len(space.shapes),)),
        out_shape=(
            jax.ShapeDtypeStruct((rhs.shape[0], points), F32),
            jax.ShapeDtypeStruct((rhs.shape[0], rank), BF16),
        ),
        in_specs=[hbm_spec] * 4,
        out_specs=(vmem_spec, vmem_spec),
        scratch_shapes=[
            pltpu.VMEM(rhs.shape, BF16),
            pltpu.VMEM(leaf_inverse.shape[1:], BF16),
            pltpu.VMEM(up_basis.shape, BF16),
            pltpu.VMEM(projection.shape, BF16),
            pltpu.VMEM((rhs.shape[0], points), BF16),
            pltpu.VMEM((levels - 1, rhs.shape[0], rank), BF16),
            pltpu.VMEM((levels * (levels + 1), rank, 2 * rank), BF16),
            pltpu.VMEM((max(len(sums), 1), rank, 2 * rank), BF16),
            pltpu.SemaphoreType.DMA((2 + 2 * levels,)),
            pltpu.SemaphoreType.DMA((CHUNKS, space.sems)),
            pltpu.SemaphoreType.DMA((CHUNKS, space.sems)),
            pltpu.SemaphoreType.DMA((max(more.sems, 1),)),
            pltpu.SemaphoreType.DMA((max(more.sems, 1),)),
        ]
        + [pltpu.VMEM(shape, F32) for _ in range(CHUNKS) for shape in space.shapes]
        + [pltpu.VMEM(shape, F32) for shape in more.shapes],
        compiler_params=pltpu.CompilerParams(
            collective_id=0, has_side_effects=True, vmem_limit_bytes=44 * 2**20
        ),
    )(*[pltpu.with_memory_space_constraint(x, pltpu.MemorySpace.HBM) for x in (rhs, leaf_inverse, up_basis, projection)])
    return state - jnp.dot(coefficient, up_basis[levels - 1], preferred_element_type=F32)


def solution(mesh):
    return jax.shard_map(
        shards,
        mesh=mesh,
        in_specs=(
            P(None, ("gy", "gx")),
            P(("gy", "gx"), None, None),
            P(None, None, ("gy", "gx")),
            P(None, None, ("gy", "gx")),
        ),
        out_specs=P(None, ("gy", "gx")),
        check_vma=False,
    )
```

```python
import functools

import jax
import jax.numpy as jnp
from jax import lax
from jax.experimental import pallas as pl
from jax.experimental.pallas import tpu as pltpu
from jax.sharding import PartitionSpec as P

CHUNKS = 4
SUBLANES = 8
F32 = jnp.float32
BF16 = jnp.bfloat16
MESH = pl.DeviceIdType.MESH


def level_plan(height, bits_x, rows):
    top = height - 1
    groups = []
    low = [b for b in range(min(top, bits_x))]
    high = [b for b in range(bits_x, top)]
    if top == bits_x:
        groups.append([top])
    elif top > bits_x:
        groups.append([bits_x])
        last = [top] + high[1:]
        if len(low) <= 3 and rows >> len(low) + len(high) >= SUBLANES:
            last, low = last + low, []
        groups.append(last)
    if top < bits_x and len(low) < 3:
        groups.append(low + [top])
    else:
        while low:
            groups.append(low[:3])
            low = low[3:]
        if top < bits_x:
            groups.append([top])
    phases = []
    for bits in groups:
        split = [b for b in bits if b != top]
        if rows >> len(split) < SUBLANES:
            assert top not in bits
            phases.append((bits, []))
        else:
            rows >>= len(split)
            phases.append((bits, split))
    return phases


def masks_of(bits):
    masks = [0]
    for b in bits:
        masks += [m | 1 << b for m in masks]
    return masks[1:]


def triples(bits):
    return [bits[i : i + 3] for i in range(0, len(bits), 3)]


def pairs(bits):
    return [bits[i : i + 2] for i in range(0, len(bits), 2)]


def sub_index(pos, bits):
    index = 0
    for k, b in enumerate(bits):
        index = index + ((pos >> b) & 1) * (1 << k)
    return index


class Step:
    def __init__(self, kind, bits, half, block, split, src, landing, dst, shape, sem):
        self.kind, self.masks = kind, masks_of(bits)
        self.half, self.block, self.split = half, block, split
        self.src, self.landing, self.dst = src, landing, dst
        self.shape, self.sem = shape, sem


class Buffers:
    def __init__(self):
        self.shapes, self.sems = [], 0

    def new(self, *shape):
        self.shapes.append(shape)
        return len(self.shapes) - 1

    def reduce(self, src, shape, bits, half=None, block=None, split=()):
        c, b, n, r = shape
        shape = (1 if half is not None else c, 1 if block is not None else b, n >> len(split), r)
        landing = self.new(2 ** len(bits) - 1, *shape)
        step = Step("reduce", bits, half, block, list(split), src, landing, self.new(*shape), shape, self.sems)
        self.sems += len(step.masks)
        return step

    def gather(self, src, shape, split, block=None):
        c, b, n, r = shape
        bits = list(split) + ([] if block is None else [block])
        whole = (c, b if block is None else 2, n << len(split), r)
        step = Step("gather", bits, None, block, list(split), src, None, self.new(*whole), shape, self.sems)
        self.sems += len(step.masks)
        return step

    def chain(self, src, shape, makers):
        steps = []
        for make in makers:
            steps.append(make(src, shape))
            src, shape = steps[-1].dst, self.shapes[steps[-1].dst]
        return steps, src, shape


def group_levels(levels, rows):
    groups, height = [], 1
    while height <= levels:
        pair = height % 2 == 0 and height < levels and rows // 2 >> height - 1 >= SUBLANES
        groups.append((height, height + 1) if pair else (height,))
        height += len(groups[-1])
    return groups


def build_plan(levels, bits_x, rows, rank):
    plan, space, tables = [], Buffers(), {}
    for group in group_levels(levels, rows):
        height = group[0]
        top = height - 1
        entry = {"group": group}
        if len(group) == 1:
            shape = (2, 1, rows, rank)
            tables[height] = space.new(*shape)
            makers, splits = [], []
            for bits, split in level_plan(height, bits_x, rows):
                half = top if top in bits else None
                makers.append(functools.partial(space.reduce, bits=bits, half=half, split=split))
                if split:
                    splits.append(split)
            entry["reduce"], src, shape = space.chain(tables[height], shape, makers)
            makers = [functools.partial(space.gather, split=s) for s in reversed(splits)]
            entry["gather"], entry["result"], _ = space.chain(src, shape, makers)
        else:
            low = list(range(top))
            shape = (2, 2, rows // 2, rank)
            first, second = space.new(*shape), space.new(*shape)
            tables[height], tables[height + 1] = first, second
            parts = [functools.partial(space.reduce, bits=g, split=g) for g in pairs(low)]
            own = functools.partial(space.reduce, bits=[top], half=top)
            entry["early"] = top == bits_x
            one, two = [own] + parts, parts
            if entry["early"]:
                nested = [b for g in reversed(pairs(low)) for b in g]
                direct = [functools.partial(space.reduce, bits=nested, split=nested)]
                two = [
                    functools.partial(space.reduce, bits=[top], block=top),
                    functools.partial(space.reduce, bits=[height], half=height),
                ] + (direct if len(low) <= 3 else parts)
            entry["one"], src, shape = space.chain(first, shape, one)
            entry["owned"], n = src, shape[2]
            makers = [functools.partial(space.gather, split=g) for g in reversed(pairs(low))]
            entry["gather_one"], entry["result_one"], _ = space.chain(src, shape, makers)
            entry["two"], entry["partial"], _ = space.chain(second, (2, 2, rows // 2, rank), two)
            shape = (2, 2, n, rank)
            entry["joined"] = space.new(*shape)
            entry["last"] = space.reduce(entry["joined"], shape, [top, height], half=height, block=top)
            shape = entry["last"].shape
            if entry["early"]:
                nested = [b for g in reversed(pairs(low)) for b in g]
                makers = [functools.partial(space.gather, split=g) for g in triples(nested)]
                makers += [functools.partial(space.gather, split=[], block=top)]
            elif len(low) < 3:
                makers = [functools.partial(space.gather, split=low, block=top)]
            else:
                makers = [functools.partial(space.gather, split=[], block=top)]
                makers += [functools.partial(space.gather, split=g) for g in reversed(pairs(low))]
            entry["gather_two"], entry["result_two"], _ = space.chain(entry["last"].dst, shape, makers)
        plan.append(entry)
    return plan, space, tables


def build_sums(plan, rank):
    space, sums = Buffers(), []
    for entry in plan:
        if len(entry["group"]) == 1:
            continue
        height = entry["group"][0]
        low = list(range(height - 1))
        shape = (2, 1, rank, rank)
        src = space.new(*shape)
        makers, splits = [], []
        for bit in low[1:]:
            makers.append(functools.partial(space.reduce, bits=[bit], split=[bit]))
            splits.append([bit])
        makers.append(functools.partial(space.reduce, bits=low[:1]))
        steps, dst, shape = space.chain(src, shape, makers)
        makers = [functools.partial(space.gather, split=s) for s in reversed(splits)]
        more, dst, _ = space.chain(dst, shape, makers)
        sums.append((height, src, steps + more, dst))
    return sums, space


def kernel(dims, plan, tables, sums, counts, rhs_hbm, leaf_hbm, up_hbm, proj_hbm, state, last_ref, last_up, *scratch):
    bits_x, bits_y, levels, chunks, rows, rank = dims
    rhs, leaf, up, proj, rounded, coef, mix, mix_sum = scratch[:8]
    in_sems, send_sems, recv_sems, sum_send, sum_recv = scratch[8:13]
    per_chunk = counts[0]
    gx, gy = lax.axis_index("gx"), lax.axis_index("gy")
    pos = gy * (1 << bits_x) + gx

    def device(mask):
        return {"gx": gx ^ (mask & ((1 << bits_x) - 1)), "gy": gy ^ (mask >> bits_x)}

    loads = {
        "rhs": pltpu.make_async_copy(rhs_hbm, rhs, in_sems.at[0]),
        "leaf": pltpu.make_async_copy(leaf_hbm.at[0], leaf, in_sems.at[1]),
    }
    for level in range(levels):
        loads["proj", level] = pltpu.make_async_copy(proj_hbm.at[level], proj.at[level], in_sems.at[2 + 2 * level])
        if level < levels - 1:
            loads["up", level] = pltpu.make_async_copy(up_hbm.at[level], up.at[level], in_sems.at[3 + 2 * level])
    loads["last_up"] = pltpu.make_async_copy(up_hbm.at[levels - 1], last_up, in_sems.at[1 + 2 * levels])
    for load in loads.values():
        load.start()

    def need(*key):
        load = loads.pop(key if len(key) > 1 else key[0], None)
        if load is not None:
            load.wait()

    greeted = {1 << b for b in range(bits_x + bits_y)}
    for entry in plan:
        group = entry["group"]
        if len(group) == 1:
            for step in entry["reduce"] + entry["gather"]:
                greeted.update(step.masks)
        elif entry["early"]:
            greeted.update(entry["last"].masks)
        else:
            for step in entry["one"]:
                greeted.update(step.masks)
    barrier = pltpu.get_barrier_semaphore()
    for mask in sorted(greeted):
        pl.semaphore_signal(barrier, inc=1, device_id=device(mask), device_id_type=MESH)

    sent = []

    def start(step, bufs, send, recv):
        src, dst = bufs[step.src], bufs[step.dst]
        n = step.shape[2]

        def piece(who):
            halves = pl.ds(0, step.shape[0]) if step.half is None else pl.ds((who >> step.half) & 1, 1)
            blocks = pl.ds(0, step.shape[1]) if step.block is None else pl.ds((who >> step.block) & 1, 1)
            return halves, blocks, pl.ds(pl.multiple_of(sub_index(who, step.split) * n, n), n)

        copies = []
        for k, mask in enumerate(step.masks):
            if step.kind == "gather":
                frm, to = src, dst.at[piece(pos)]
            else:
                frm, to = src.at[piece(pos ^ mask)], bufs[step.landing].at[k]
            copy = pltpu.make_async_remote_copy(
                src_ref=frm,
                dst_ref=to,
                send_sem=send(step.sem + k),
                recv_sem=recv(step.sem + k),
                device_id=device(mask),
                device_id_type=MESH,
            )
            copy.start()
            copies.append(copy)
        sent.extend(copies)
        if step.kind == "gather":
            dst[piece(pos)] = src[...]

        def finish():
            for copy in copies:
                copy.wait_recv()
            if step.kind == "reduce":
                total = src[piece(pos)]
                for k in range(len(step.masks)):
                    total = total + bufs[step.landing][k]
                dst[...] = total

        return finish

    def mixing(low, high):
        return low * levels + high

    def flow(chunk):
        lo = chunk * rows
        bufs = scratch[13 + chunk * per_chunk : 13 + (chunk + 1) * per_chunk]
        span = slice(lo, lo + rows)

        def begin(step):
            return start(step, bufs, lambda k: send_sems.at[chunk, k], lambda k: recv_sems.at[chunk, k])

        def project(height):
            need("proj", height - 1)
            table = bufs[tables[height]]
            for half in range(2):
                value = lax.dot_general(
                    rounded[span, :],
                    proj[height - 1, half * rank : (half + 1) * rank, :],
                    (((1,), (1,)), ((), ())),
                    preferred_element_type=F32,
                )
                table[half] = value.reshape(table.shape[1:])

        def keep(height, ref):
            value = ref[0].reshape(rows, rank).astype(BF16)
            if height == levels:
                last_ref[span, :] = value
            else:
                coef[height - 1, span, :] = value

        def correct(done, heights):
            for height in heights:
                delta = jnp.dot(coef[done - 1, span, :], mix[mixing(done, height)], preferred_element_type=F32)
                table = bufs[tables[height]]
                for half in range(2):
                    part = delta[:, half * rank : (half + 1) * rank]
                    table[half] = table[half] - part.reshape(table.shape[1:])

        def update(heights):
            value = state[span, :]
            for height in heights:
                need("up", height - 1)
                value = value - jnp.dot(coef[height - 1, span, :], up[height - 1], preferred_element_type=F32)
            state[span, :] = value

        need("rhs")
        need("leaf")
        value = jnp.dot(rhs[span, :], leaf[...], preferred_element_type=F32)
        state[span, :] = value
        rounded[span, :] = value.astype(BF16)
        project(1)
        if chunk == 0:
            pl.semaphore_wait(barrier, len(greeted))

        later = []
        for index, entry in enumerate(plan):
            group = entry["group"]
            after = [h for e in plan[index + 1 : index + 2] for h in e["group"]]
            beyond = [h for e in plan[index + 2 :] for h in e["group"]]
            if len(group) == 1:
                height = group[0]
                for step in entry["reduce"] + entry["gather"]:
                    finish = begin(step)
                    for work in later:
                        work()
                    later = []
                    yield
                    if height == 1 and step is entry["reduce"][0]:
                        for other in range(2, levels + 1):
                            project(other)
                    finish()
                keep(height, bufs[entry["result"]])
                if height < levels:
                    correct(height, after)
                    later = [functools.partial(correct, height, beyond), functools.partial(update, [height])]
            else:
                height = group[0]
                one, two = entry["one"], entry["two"]
                first, second = begin(one[0]), begin(two[0])
                for work in later:
                    work()
                later = []
                ahead = len(two) if not entry["early"] else min(len(two), len(one)) - 1
                at = 0
                for i in range(max(len(one), ahead)):
                    yield
                    if i < len(one):
                        first()
                        if i + 1 < len(one):
                            first = begin(one[i + 1])
                        else:
                            fetch = begin(entry["gather_one"][0])
                    if at < ahead:
                        second()
                        at += 1
                        if at < len(two):
                            second = begin(two[at])
                owned, joined, base = bufs[entry["owned"]], bufs[entry["joined"]], bufs[entry["partial"]]
                n = owned.shape[2]
                complete(height)
                table = mix_sum[[s[0] for s in sums].index(height)]
                delta = jnp.dot(owned[0].reshape(2 * n, rank).astype(BF16), table, preferred_element_type=F32)
                for half in range(2):
                    for block in range(2):
                        part = delta[block * n : (block + 1) * n, half * rank : (half + 1) * rank]
                        if entry["early"]:
                            joined[half, block] = -part
                        else:
                            joined[half, block] = base[half, block] - part
                finish = begin(entry["last"])
                yield
                while at < len(two):
                    second()
                    at += 1
                    if at < len(two):
                        second = begin(two[at])
                finish()
                if entry["early"]:
                    end = bufs[entry["last"].dst]
                    end[...] = end[...] + base[...]
                finish = begin(entry["gather_two"][0])
                fetch()
                for step in entry["gather_one"][1:]:
                    fetch = begin(step)
                    yield
                    fetch()
                keep(height, bufs[entry["result_one"]])
                correct(height, after)
                later = [functools.partial(correct, height, beyond)]
                if after:
                    later.append(functools.partial(correct, height + 1, beyond))
                    later.append(functools.partial(update, [height, height + 1]))
                else:
                    update([height])
                    later = []
                yield
                finish()
                for step in entry["gather_two"][1:]:
                    finish = begin(step)
                    yield
                    finish()
                keep(height + 1, bufs[entry["result_two"]])
                if after:
                    correct(height + 1, after)

    sum_bufs = scratch[13 + chunks * per_chunk :]
    running = {}

    def compute(low, high):
        need("up", low - 1)
        need("proj", high - 1)
        value = lax.dot_general(up[low - 1], proj[high - 1], (((1,), (1,)), ((), ())), preferred_element_type=F32)
        mix[mixing(low, high)] = value.astype(BF16)
        return value

    def advance(height):
        for k, (key, src, steps, dst) in enumerate(sums):
            if key != height:
                continue
            if height in running:
                at, finish = running[height]
                if finish is None:
                    return
                finish()
            else:
                at = -1
            at += 1
            if at < len(steps):
                begun = start(steps[at], sum_bufs, lambda i: sum_send.at[i], lambda i: sum_recv.at[i])
                running[height] = (at, begun)
            else:
                running[height] = (at, None)
                for half in range(2):
                    mix_sum[k, :, half * rank : (half + 1) * rank] = sum_bufs[dst][half, 0].astype(BF16)

    def complete(height):
        while running.get(height, (0, 0))[1] is not None:
            advance(height)

    def summing():
        for low in range(1, levels):
            for high in range(low + 1, levels + 1):
                value = compute(low, high)
                for height, src, _, _ in sums:
                    if (low, high) == (height, height + 1):
                        for half in range(2):
                            sum_bufs[src][half, 0] = value[:, half * rank : (half + 1) * rank]
        for height, _, _, _ in sums[1:]:
            advance(height)
        yield
        for _ in range(max([0] + [len(steps) + 1 for _, _, steps, _ in sums])):
            for height, _, _, _ in sums:
                advance(height)
            yield

    flows = [flow(chunk) for chunk in range(chunks)] + [summing()]
    while flows:
        left = []
        for item in flows:
            try:
                next(item)
                left.append(item)
            except StopIteration:
                pass
        flows = left
    for copy in sent:
        copy.wait_send()
    for key in list(loads):
        loads.pop(key).wait()


def finish_kernel(parts, state, coef, up, out_hbm, value, sems):
    rows = state.shape[0] // parts
    copies = []
    for part in range(parts):
        span = slice(part * rows, (part + 1) * rows)
        value[span, :] = state[span, :] - jnp.dot(coef[span, :], up[...], preferred_element_type=F32)
        copy = pltpu.make_async_copy(value.at[span], out_hbm.at[span], sems.at[part])
        copy.start()
        copies.append(copy)
    for copy in copies:
        copy.wait()


def shards(rhs, leaf_inverse, up_basis, projection):
    bits_x = lax.axis_size("gx").bit_length() - 1
    bits_y = lax.axis_size("gy").bit_length() - 1
    levels, rank, points = up_basis.shape
    rows = rhs.shape[0] // CHUNKS
    plan, space, tables = build_plan(levels, bits_x, rows, rank)
    sums, more = build_sums(plan, rank)
    dims = (bits_x, bits_y, levels, CHUNKS, rows, rank)
    hbm_spec = pl.BlockSpec(memory_space=pltpu.MemorySpace.HBM)
    vmem_spec = pl.BlockSpec(memory_space=pltpu.VMEM)
    state, coefficient, last_up = pl.pallas_call(
        functools.partial(kernel, dims, plan, tables, sums, (len(space.shapes),)),
        out_shape=(
            jax.ShapeDtypeStruct((rhs.shape[0], points), F32),
            jax.ShapeDtypeStruct((rhs.shape[0], rank), BF16),
            jax.ShapeDtypeStruct((rank, points), BF16),
        ),
        in_specs=[hbm_spec] * 4,
        out_specs=(vmem_spec, vmem_spec, vmem_spec),
        scratch_shapes=[
            pltpu.VMEM(rhs.shape, BF16),
            pltpu.VMEM(leaf_inverse.shape[1:], BF16),
            pltpu.VMEM(up_basis.shape, BF16),
            pltpu.VMEM(projection.shape, BF16),
            pltpu.VMEM((rhs.shape[0], points), BF16),
            pltpu.VMEM((levels - 1, rhs.shape[0], rank), BF16),
            pltpu.VMEM((levels * (levels + 1), rank, 2 * rank), BF16),
            pltpu.VMEM((max(len(sums), 1), rank, 2 * rank), BF16),
            pltpu.SemaphoreType.DMA((2 + 2 * levels,)),
            pltpu.SemaphoreType.DMA((CHUNKS, space.sems)),
            pltpu.SemaphoreType.DMA((CHUNKS, space.sems)),
            pltpu.SemaphoreType.DMA((max(more.sems, 1),)),
            pltpu.SemaphoreType.DMA((max(more.sems, 1),)),
        ]
        + [pltpu.VMEM(shape, F32) for _ in range(CHUNKS) for shape in space.shapes]
        + [pltpu.VMEM(shape, F32) for shape in more.shapes],
        compiler_params=pltpu.CompilerParams(
            collective_id=0, has_side_effects=True, vmem_limit_bytes=44 * 2**20
        ),
    )(*[pltpu.with_memory_space_constraint(x, pltpu.MemorySpace.HBM) for x in (rhs, leaf_inverse, up_basis, projection)])
    parts = 4
    return pl.pallas_call(
        functools.partial(finish_kernel, parts),
        out_shape=jax.ShapeDtypeStruct(state.shape, F32),
        in_specs=[vmem_spec] * 3,
        out_specs=pl.BlockSpec(memory_space=pl.ANY),
        scratch_shapes=[pltpu.VMEM(state.shape, F32), pltpu.SemaphoreType.DMA((parts,))],
        compiler_params=pltpu.CompilerParams(vmem_limit_bytes=8 * 2**20),
    )(state, coefficient, last_up)


def solution(mesh):
    return jax.shard_map(
        shards,
        mesh=mesh,
        in_specs=(
            P(None, ("gy", "gx")),
            P(("gy", "gx"), None, None),
            P(None, None, ("gy", "gx")),
            P(None, None, ("gy", "gx")),
        ),
        out_specs=P(None, ("gy", "gx")),
        check_vma=False,
    )
```

```python
import functools

import jax
import jax.numpy as jnp
from jax import lax
from jax.experimental import pallas as pl
from jax.experimental.pallas import tpu as pltpu
from jax.sharding import PartitionSpec as P

CHUNKS = 4
SUBLANES = 8
F32 = jnp.float32
BF16 = jnp.bfloat16
MESH = pl.DeviceIdType.MESH


def level_plan(height, bits_x, rows):
    top = height - 1
    groups = []
    low = [b for b in range(min(top, bits_x))]
    high = [b for b in range(bits_x, top)]
    if top == bits_x:
        groups.append([top])
    elif top > bits_x:
        groups.append([bits_x])
        last = [top] + high[1:]
        if len(low) <= 3 and rows >> len(low) + len(high) >= SUBLANES:
            last, low = last + low, []
        groups.append(last)
    if top < bits_x and len(low) < 3:
        groups.append(low + [top])
    else:
        while low:
            groups.append(low[:3])
            low = low[3:]
        if top < bits_x:
            groups.append([top])
    phases = []
    for bits in groups:
        split = [b for b in bits if b != top]
        if rows >> len(split) < SUBLANES:
            assert top not in bits
            phases.append((bits, []))
        else:
            rows >>= len(split)
            phases.append((bits, split))
    return phases


def masks_of(bits):
    masks = [0]
    for b in bits:
        masks += [m | 1 << b for m in masks]
    return masks[1:]


def triples(bits):
    return [bits[i : i + 3] for i in range(0, len(bits), 3)]


def pairs(bits):
    return [bits[i : i + 2] for i in range(0, len(bits), 2)]


def sub_index(pos, bits):
    index = 0
    for k, b in enumerate(bits):
        index = index + ((pos >> b) & 1) * (1 << k)
    return index


class Step:
    def __init__(self, kind, bits, half, block, split, src, landing, dst, shape, sem):
        self.kind, self.masks = kind, masks_of(bits)
        self.half, self.block, self.split = half, block, split
        self.src, self.landing, self.dst = src, landing, dst
        self.shape, self.sem = shape, sem


class Buffers:
    def __init__(self):
        self.shapes, self.sems = [], 0

    def new(self, *shape):
        self.shapes.append(shape)
        return len(self.shapes) - 1

    def reduce(self, src, shape, bits, half=None, block=None, split=()):
        c, b, n, r = shape
        shape = (1 if half is not None else c, 1 if block is not None else b, n >> len(split), r)
        landing = self.new(2 ** len(bits) - 1, *shape)
        step = Step("reduce", bits, half, block, list(split), src, landing, self.new(*shape), shape, self.sems)
        self.sems += len(step.masks)
        return step

    def gather(self, src, shape, split, block=None):
        c, b, n, r = shape
        bits = list(split) + ([] if block is None else [block])
        whole = (c, b if block is None else 2, n << len(split), r)
        step = Step("gather", bits, None, block, list(split), src, None, self.new(*whole), shape, self.sems)
        self.sems += len(step.masks)
        return step

    def chain(self, src, shape, makers):
        steps = []
        for make in makers:
            steps.append(make(src, shape))
            src, shape = steps[-1].dst, self.shapes[steps[-1].dst]
        return steps, src, shape


def group_levels(levels, rows):
    groups, height = [], 1
    while height <= levels:
        pair = height % 2 == 0 and height < levels and rows // 2 >> height - 1 >= SUBLANES
        groups.append((height, height + 1) if pair else (height,))
        height += len(groups[-1])
    return groups


def build_plan(levels, bits_x, rows, rank):
    plan, space, tables = [], Buffers(), {}
    for group in group_levels(levels, rows):
        height = group[0]
        top = height - 1
        entry = {"group": group}
        if len(group) == 1:
            shape = (2, 1, rows, rank)
            tables[height] = space.new(*shape)
            makers, splits = [], []
            for bits, split in level_plan(height, bits_x, rows):
                half = top if top in bits else None
                makers.append(functools.partial(space.reduce, bits=bits, half=half, split=split))
                if split:
                    splits.append(split)
            entry["reduce"], src, shape = space.chain(tables[height], shape, makers)
            makers = [functools.partial(space.gather, split=s) for s in reversed(splits)]
            entry["gather"], entry["result"], _ = space.chain(src, shape, makers)
        else:
            low = list(range(top))
            shape = (2, 2, rows // 2, rank)
            first, second = space.new(*shape), space.new(*shape)
            tables[height], tables[height + 1] = first, second
            parts = [functools.partial(space.reduce, bits=g, split=g) for g in pairs(low)]
            own = functools.partial(space.reduce, bits=[top], half=top)
            entry["early"] = top == bits_x
            one, two = [own] + parts, parts
            if entry["early"]:
                nested = [b for g in reversed(pairs(low)) for b in g]
                direct = [functools.partial(space.reduce, bits=nested, split=nested)]
                two = [
                    functools.partial(space.reduce, bits=[top], block=top),
                    functools.partial(space.reduce, bits=[height], half=height),
                ] + (direct if len(low) <= 3 else parts)
            entry["one"], src, shape = space.chain(first, shape, one)
            entry["owned"], n = src, shape[2]
            makers = [functools.partial(space.gather, split=g) for g in reversed(pairs(low))]
            entry["gather_one"], entry["result_one"], _ = space.chain(src, shape, makers)
            entry["two"], entry["partial"], _ = space.chain(second, (2, 2, rows // 2, rank), two)
            shape = (2, 2, n, rank)
            entry["joined"] = space.new(*shape)
            entry["last"] = space.reduce(entry["joined"], shape, [top, height], half=height, block=top)
            shape = entry["last"].shape
            if entry["early"]:
                nested = [b for g in reversed(pairs(low)) for b in g]
                makers = [functools.partial(space.gather, split=g) for g in triples(nested)]
                makers += [functools.partial(space.gather, split=[], block=top)]
            elif len(low) < 3:
                makers = [functools.partial(space.gather, split=low, block=top)]
            else:
                makers = [functools.partial(space.gather, split=[], block=top)]
                makers += [functools.partial(space.gather, split=g) for g in reversed(pairs(low))]
            entry["gather_two"], entry["result_two"], _ = space.chain(entry["last"].dst, shape, makers)
        plan.append(entry)
    return plan, space, tables


def build_sums(plan, rank):
    space, sums = Buffers(), []
    for entry in plan:
        if len(entry["group"]) == 1:
            continue
        height = entry["group"][0]
        low = list(range(height - 1))
        shape = (2, 1, rank, rank)
        src = space.new(*shape)
        makers, splits = [], []
        for bit in low[1:]:
            makers.append(functools.partial(space.reduce, bits=[bit], split=[bit]))
            splits.append([bit])
        makers.append(functools.partial(space.reduce, bits=low[:1]))
        steps, dst, shape = space.chain(src, shape, makers)
        makers = [functools.partial(space.gather, split=s) for s in reversed(splits)]
        more, dst, _ = space.chain(dst, shape, makers)
        sums.append((height, src, steps + more, dst))
    return sums, space


def kernel(dims, plan, tables, sums, counts, rhs_hbm, leaf_hbm, up_hbm, proj_hbm, state, last_ref, last_up, *scratch):
    bits_x, bits_y, levels, chunks, rows, rank = dims
    rhs, leaf, up, proj, rounded, coef, mix, mix_sum = scratch[:8]
    in_sems, send_sems, recv_sems, sum_send, sum_recv = scratch[8:13]
    per_chunk = counts[0]
    gx, gy = lax.axis_index("gx"), lax.axis_index("gy")
    pos = gy * (1 << bits_x) + gx

    def device(mask):
        return {"gx": gx ^ (mask & ((1 << bits_x) - 1)), "gy": gy ^ (mask >> bits_x)}

    loads = {
        "rhs": pltpu.make_async_copy(rhs_hbm, rhs, in_sems.at[0]),
        "leaf": pltpu.make_async_copy(leaf_hbm.at[0], leaf, in_sems.at[1]),
    }
    for level in range(levels):
        loads["proj", level] = pltpu.make_async_copy(proj_hbm.at[level], proj.at[level], in_sems.at[2 + 2 * level])
        if level < levels - 1:
            loads["up", level] = pltpu.make_async_copy(up_hbm.at[level], up.at[level], in_sems.at[3 + 2 * level])
    loads["last_up"] = pltpu.make_async_copy(up_hbm.at[levels - 1], last_up, in_sems.at[1 + 2 * levels])
    for load in loads.values():
        load.start()

    def need(*key):
        load = loads.pop(key if len(key) > 1 else key[0], None)
        if load is not None:
            load.wait()

    greeted = {1 << b for b in range(bits_x + bits_y)}
    for entry in plan:
        group = entry["group"]
        if len(group) == 1:
            for step in entry["reduce"] + entry["gather"]:
                greeted.update(step.masks)
        elif entry["early"]:
            greeted.update(entry["last"].masks)
        else:
            for step in entry["one"]:
                greeted.update(step.masks)
    barrier = pltpu.get_barrier_semaphore()
    for mask in sorted(greeted):
        pl.semaphore_signal(barrier, inc=1, device_id=device(mask), device_id_type=MESH)

    sent, idle = [], []

    def start(step, bufs, send, recv):
        src, dst = bufs[step.src], bufs[step.dst]
        n = step.shape[2]

        def piece(who):
            halves = pl.ds(0, step.shape[0]) if step.half is None else pl.ds((who >> step.half) & 1, 1)
            blocks = pl.ds(0, step.shape[1]) if step.block is None else pl.ds((who >> step.block) & 1, 1)
            return halves, blocks, pl.ds(pl.multiple_of(sub_index(who, step.split) * n, n), n)

        copies = []
        for k, mask in enumerate(step.masks):
            if step.kind == "gather":
                frm, to = src, dst.at[piece(pos)]
            else:
                frm, to = src.at[piece(pos ^ mask)], bufs[step.landing].at[k]
            copy = pltpu.make_async_remote_copy(
                src_ref=frm,
                dst_ref=to,
                send_sem=send(step.sem + k),
                recv_sem=recv(step.sem + k),
                device_id=device(mask),
                device_id_type=MESH,
            )
            copy.start()
            copies.append(copy)
        sent.extend(copies)
        if step.kind == "gather":
            dst[piece(pos)] = src[...]

        def finish():
            for copy in copies:
                copy.wait_recv()
            if step.kind == "reduce":
                total = src[piece(pos)]
                for k in range(len(step.masks)):
                    total = total + bufs[step.landing][k]
                dst[...] = total

        return finish

    def mixing(low, high):
        return low * levels + high

    def flow(chunk):
        lo = chunk * rows
        bufs = scratch[13 + chunk * per_chunk : 13 + (chunk + 1) * per_chunk]
        span = slice(lo, lo + rows)

        def begin(step):
            return start(step, bufs, lambda k: send_sems.at[chunk, k], lambda k: recv_sems.at[chunk, k])

        def project(height):
            need("proj", height - 1)
            table = bufs[tables[height]]
            for half in range(2):
                value = lax.dot_general(
                    rounded[span, :],
                    proj[height - 1, half * rank : (half + 1) * rank, :],
                    (((1,), (1,)), ((), ())),
                    preferred_element_type=F32,
                )
                table[half] = value.reshape(table.shape[1:])

        def keep(height, ref):
            value = ref[0].reshape(rows, rank).astype(BF16)
            if height == levels:
                last_ref[span, :] = value
            else:
                coef[height - 1, span, :] = value

        def correct(done, heights):
            for height in heights:
                delta = jnp.dot(coef[done - 1, span, :], mix[mixing(done, height)], preferred_element_type=F32)
                table = bufs[tables[height]]
                for half in range(2):
                    part = delta[:, half * rank : (half + 1) * rank]
                    table[half] = table[half] - part.reshape(table.shape[1:])

        def update(heights):
            value = state[span, :]
            for height in heights:
                need("up", height - 1)
                value = value - jnp.dot(coef[height - 1, span, :], up[height - 1], preferred_element_type=F32)
            state[span, :] = value

        need("rhs")
        need("leaf")
        value = jnp.dot(rhs[span, :], leaf[...], preferred_element_type=F32)
        state[span, :] = value
        rounded[span, :] = value.astype(BF16)
        project(1)
        if chunk == 0:
            pl.semaphore_wait(barrier, len(greeted))

        later = []
        for index, entry in enumerate(plan):
            group = entry["group"]
            after = [h for e in plan[index + 1 : index + 2] for h in e["group"]]
            beyond = [h for e in plan[index + 2 :] for h in e["group"]]
            if len(group) == 1:
                height = group[0]
                for step in entry["reduce"] + entry["gather"]:
                    finish = begin(step)
                    idle.extend(later)
                    later = []
                    yield
                    if height == 1 and step is entry["reduce"][0]:
                        for other in range(2, levels + 1):
                            project(other)
                    finish()
                keep(height, bufs[entry["result"]])
                if height < levels:
                    correct(height, after)
                    later = [functools.partial(correct, height, beyond), functools.partial(update, [height])]
            else:
                height = group[0]
                one, two = entry["one"], entry["two"]
                first, second = begin(one[0]), begin(two[0])
                idle.extend(later)
                later = []
                ahead = len(two) if not entry["early"] else min(len(two), len(one)) - 1
                at = 0
                for i in range(max(len(one), ahead)):
                    yield
                    if i < len(one):
                        first()
                        if i + 1 < len(one):
                            first = begin(one[i + 1])
                        else:
                            fetch = begin(entry["gather_one"][0])
                    if at < ahead:
                        second()
                        at += 1
                        if at < len(two):
                            second = begin(two[at])
                owned, joined, base = bufs[entry["owned"]], bufs[entry["joined"]], bufs[entry["partial"]]
                n = owned.shape[2]
                complete(height)
                table = mix_sum[[s[0] for s in sums].index(height)]
                delta = jnp.dot(owned[0].reshape(2 * n, rank).astype(BF16), table, preferred_element_type=F32)
                for half in range(2):
                    for block in range(2):
                        part = delta[block * n : (block + 1) * n, half * rank : (half + 1) * rank]
                        if entry["early"]:
                            joined[half, block] = -part
                        else:
                            joined[half, block] = base[half, block] - part
                finish = begin(entry["last"])
                yield
                while at < len(two):
                    second()
                    at += 1
                    if at < len(two):
                        second = begin(two[at])
                finish()
                if entry["early"]:
                    end = bufs[entry["last"].dst]
                    end[...] = end[...] + base[...]
                finish = begin(entry["gather_two"][0])
                fetch()
                for step in entry["gather_one"][1:]:
                    fetch = begin(step)
                    yield
                    fetch()
                keep(height, bufs[entry["result_one"]])
                correct(height, after)
                later = [functools.partial(correct, height, beyond)]
                if after:
                    later.append(functools.partial(correct, height + 1, beyond))
                    later.append(functools.partial(update, [height, height + 1]))
                else:
                    update([height])
                    later = []
                yield
                finish()
                for step in entry["gather_two"][1:]:
                    finish = begin(step)
                    yield
                    finish()
                keep(height + 1, bufs[entry["result_two"]])
                if after:
                    correct(height + 1, after)

    sum_bufs = scratch[13 + chunks * per_chunk :]
    running = {}

    def compute(low, high):
        need("up", low - 1)
        need("proj", high - 1)
        value = lax.dot_general(up[low - 1], proj[high - 1], (((1,), (1,)), ((), ())), preferred_element_type=F32)
        mix[mixing(low, high)] = value.astype(BF16)
        return value

    def advance(height):
        for k, (key, src, steps, dst) in enumerate(sums):
            if key != height:
                continue
            if height in running:
                at, finish = running[height]
                if finish is None:
                    return
                finish()
            else:
                at = -1
            at += 1
            if at < len(steps):
                begun = start(steps[at], sum_bufs, lambda i: sum_send.at[i], lambda i: sum_recv.at[i])
                running[height] = (at, begun)
            else:
                running[height] = (at, None)
                for half in range(2):
                    mix_sum[k, :, half * rank : (half + 1) * rank] = sum_bufs[dst][half, 0].astype(BF16)

    def complete(height):
        while running.get(height, (0, 0))[1] is not None:
            advance(height)

    def summing():
        for low in range(1, levels):
            for high in range(low + 1, levels + 1):
                value = compute(low, high)
                for height, src, _, _ in sums:
                    if (low, high) == (height, height + 1):
                        for half in range(2):
                            sum_bufs[src][half, 0] = value[:, half * rank : (half + 1) * rank]
        for height, _, _, _ in sums:
            advance(height)
        yield
        for _ in range(max([0] + [len(steps) + 1 for _, _, steps, _ in sums])):
            for height, _, _, _ in sums:
                advance(height)
            yield

    flows = [flow(chunk) for chunk in range(chunks)] + [summing()]
    while flows:
        left = []
        for item in flows:
            try:
                next(item)
                left.append(item)
            except StopIteration:
                pass
        flows = left
        while idle:
            idle.pop(0)()
    for copy in sent:
        copy.wait_send()
    for key in list(loads):
        loads.pop(key).wait()


def finish_kernel(parts, state, coef, up, out_hbm, value, sems):
    rows = state.shape[0] // parts
    copies = []
    for part in range(parts):
        span = slice(part * rows, (part + 1) * rows)
        value[span, :] = state[span, :] - jnp.dot(coef[span, :], up[...], preferred_element_type=F32)
        copy = pltpu.make_async_copy(value.at[span], out_hbm.at[span], sems.at[part])
        copy.start()
        copies.append(copy)
    for copy in copies:
        copy.wait()


def shards(rhs, leaf_inverse, up_basis, projection):
    bits_x = lax.axis_size("gx").bit_length() - 1
    bits_y = lax.axis_size("gy").bit_length() - 1
    levels, rank, points = up_basis.shape
    rows = rhs.shape[0] // CHUNKS
    plan, space, tables = build_plan(levels, bits_x, rows, rank)
    sums, more = build_sums(plan, rank)
    dims = (bits_x, bits_y, levels, CHUNKS, rows, rank)
    hbm_spec = pl.BlockSpec(memory_space=pltpu.MemorySpace.HBM)
    vmem_spec = pl.BlockSpec(memory_space=pltpu.VMEM)
    state, coefficient, last_up = pl.pallas_call(
        functools.partial(kernel, dims, plan, tables, sums, (len(space.shapes),)),
        out_shape=(
            jax.ShapeDtypeStruct((rhs.shape[0], points), F32),
            jax.ShapeDtypeStruct((rhs.shape[0], rank), BF16),
            jax.ShapeDtypeStruct((rank, points), BF16),
        ),
        in_specs=[hbm_spec] * 4,
        out_specs=(vmem_spec, vmem_spec, vmem_spec),
        scratch_shapes=[
            pltpu.VMEM(rhs.shape, BF16),
            pltpu.VMEM(leaf_inverse.shape[1:], BF16),
            pltpu.VMEM(up_basis.shape, BF16),
            pltpu.VMEM(projection.shape, BF16),
            pltpu.VMEM((rhs.shape[0], points), BF16),
            pltpu.VMEM((levels - 1, rhs.shape[0], rank), BF16),
            pltpu.VMEM((levels * (levels + 1), rank, 2 * rank), BF16),
            pltpu.VMEM((max(len(sums), 1), rank, 2 * rank), BF16),
            pltpu.SemaphoreType.DMA((2 + 2 * levels,)),
            pltpu.SemaphoreType.DMA((CHUNKS, space.sems)),
            pltpu.SemaphoreType.DMA((CHUNKS, space.sems)),
            pltpu.SemaphoreType.DMA((max(more.sems, 1),)),
            pltpu.SemaphoreType.DMA((max(more.sems, 1),)),
        ]
        + [pltpu.VMEM(shape, F32) for _ in range(CHUNKS) for shape in space.shapes]
        + [pltpu.VMEM(shape, F32) for shape in more.shapes],
        compiler_params=pltpu.CompilerParams(
            collective_id=0, has_side_effects=True, vmem_limit_bytes=44 * 2**20
        ),
    )(*[pltpu.with_memory_space_constraint(x, pltpu.MemorySpace.HBM) for x in (rhs, leaf_inverse, up_basis, projection)])
    parts = 8
    return pl.pallas_call(
        functools.partial(finish_kernel, parts),
        out_shape=jax.ShapeDtypeStruct(state.shape, F32),
        in_specs=[vmem_spec] * 3,
        out_specs=pl.BlockSpec(memory_space=pl.ANY),
        scratch_shapes=[pltpu.VMEM(state.shape, F32), pltpu.SemaphoreType.DMA((parts,))],
        compiler_params=pltpu.CompilerParams(vmem_limit_bytes=8 * 2**20),
    )(state, coefficient, last_up)


def solution(mesh):
    return jax.shard_map(
        shards,
        mesh=mesh,
        in_specs=(
            P(None, ("gy", "gx")),
            P(("gy", "gx"), None, None),
            P(None, None, ("gy", "gx")),
            P(None, None, ("gy", "gx")),
        ),
        out_specs=P(None, ("gy", "gx")),
        check_vma=False,
    )
```

```python
import functools

import jax
import jax.numpy as jnp
from jax import lax
from jax.experimental import pallas as pl
from jax.experimental.pallas import tpu as pltpu
from jax.sharding import PartitionSpec as P

CHUNKS = 4
SUBLANES = 8
F32 = jnp.float32
BF16 = jnp.bfloat16
MESH = pl.DeviceIdType.MESH


def level_plan(height, bits_x, rows):
    top = height - 1
    groups = []
    low = [b for b in range(min(top, bits_x))]
    high = [b for b in range(bits_x, top)]
    if top == bits_x:
        groups.append([top])
    elif top > bits_x:
        groups.append([bits_x])
        last = [top] + high[1:]
        if len(low) <= 3 and rows >> len(low) + len(high) >= SUBLANES:
            last, low = last + low, []
        groups.append(last)
    if top < bits_x and len(low) < 3:
        groups.append(low + [top])
    else:
        while low:
            groups.append(low[:3])
            low = low[3:]
        if top < bits_x:
            groups.append([top])
    phases = []
    for bits in groups:
        split = [b for b in bits if b != top]
        if rows >> len(split) < SUBLANES:
            assert top not in bits
            phases.append((bits, []))
        else:
            rows >>= len(split)
            phases.append((bits, split))
    return phases


def masks_of(bits):
    masks = [0]
    for b in bits:
        masks += [m | 1 << b for m in masks]
    return masks[1:]


def triples(bits):
    return [bits[i : i + 3] for i in range(0, len(bits), 3)]


def pairs(bits):
    return [bits[i : i + 2] for i in range(0, len(bits), 2)]


def sub_index(pos, bits):
    index = 0
    for k, b in enumerate(bits):
        index = index + ((pos >> b) & 1) * (1 << k)
    return index


class Step:
    def __init__(self, kind, bits, half, block, split, src, landing, dst, shape, sem):
        self.kind, self.masks = kind, masks_of(bits)
        self.half, self.block, self.split = half, block, split
        self.src, self.landing, self.dst = src, landing, dst
        self.shape, self.sem = shape, sem


class Buffers:
    def __init__(self):
        self.shapes, self.sems = [], 0

    def new(self, *shape):
        self.shapes.append(shape)
        return len(self.shapes) - 1

    def reduce(self, src, shape, bits, half=None, block=None, split=()):
        c, b, n, r = shape
        shape = (1 if half is not None else c, 1 if block is not None else b, n >> len(split), r)
        landing = self.new(2 ** len(bits) - 1, *shape)
        step = Step("reduce", bits, half, block, list(split), src, landing, self.new(*shape), shape, self.sems)
        self.sems += len(step.masks)
        return step

    def gather(self, src, shape, split, block=None):
        c, b, n, r = shape
        bits = list(split) + ([] if block is None else [block])
        whole = (c, b if block is None else 2, n << len(split), r)
        step = Step("gather", bits, None, block, list(split), src, None, self.new(*whole), shape, self.sems)
        self.sems += len(step.masks)
        return step

    def chain(self, src, shape, makers):
        steps = []
        for make in makers:
            steps.append(make(src, shape))
            src, shape = steps[-1].dst, self.shapes[steps[-1].dst]
        return steps, src, shape


def group_levels(levels, rows):
    groups, height = [], 1
    while height <= levels:
        pair = height % 2 == 0 and height < levels and rows // 2 >> height - 1 >= SUBLANES
        groups.append((height, height + 1) if pair else (height,))
        height += len(groups[-1])
    return groups


def build_plan(levels, bits_x, rows, rank):
    plan, space, tables = [], Buffers(), {}
    for group in group_levels(levels, rows):
        height = group[0]
        top = height - 1
        entry = {"group": group}
        if len(group) == 1:
            shape = (2, 1, rows, rank)
            tables[height] = space.new(*shape)
            makers, splits = [], []
            for bits, split in level_plan(height, bits_x, rows):
                half = top if top in bits else None
                makers.append(functools.partial(space.reduce, bits=bits, half=half, split=split))
                if split:
                    splits.append(split)
            entry["reduce"], src, shape = space.chain(tables[height], shape, makers)
            makers = [functools.partial(space.gather, split=s) for s in reversed(splits)]
            entry["gather"], entry["result"], _ = space.chain(src, shape, makers)
        else:
            low = list(range(top))
            shape = (2, 2, rows // 2, rank)
            first, second = space.new(*shape), space.new(*shape)
            tables[height], tables[height + 1] = first, second
            parts = [functools.partial(space.reduce, bits=g, split=g) for g in pairs(low)]
            own = functools.partial(space.reduce, bits=[top], half=top)
            entry["early"] = top == bits_x
            one, two = [own] + parts, parts
            if entry["early"]:
                nested = [b for g in reversed(pairs(low)) for b in g]
                direct = [functools.partial(space.reduce, bits=nested, split=nested)]
                two = [
                    functools.partial(space.reduce, bits=[top], block=top),
                    functools.partial(space.reduce, bits=[height], half=height),
                ] + (direct if len(low) <= 3 else parts)
            entry["one"], src, shape = space.chain(first, shape, one)
            entry["owned"], n = src, shape[2]
            makers = [functools.partial(space.gather, split=g) for g in reversed(pairs(low))]
            entry["gather_one"], entry["result_one"], _ = space.chain(src, shape, makers)
            entry["two"], entry["partial"], _ = space.chain(second, (2, 2, rows // 2, rank), two)
            shape = (2, 2, n, rank)
            entry["joined"] = space.new(*shape)
            entry["last"] = space.reduce(entry["joined"], shape, [top, height], half=height, block=top)
            shape = entry["last"].shape
            if entry["early"]:
                nested = [b for g in reversed(pairs(low)) for b in g]
                makers = [functools.partial(space.gather, split=g) for g in triples(nested)]
                makers += [functools.partial(space.gather, split=[], block=top)]
            elif len(low) < 3:
                makers = [functools.partial(space.gather, split=low, block=top)]
            else:
                makers = [functools.partial(space.gather, split=[], block=top)]
                makers += [functools.partial(space.gather, split=g) for g in reversed(pairs(low))]
            entry["gather_two"], entry["result_two"], _ = space.chain(entry["last"].dst, shape, makers)
        plan.append(entry)
    return plan, space, tables


def build_sums(plan, rank):
    space, sums = Buffers(), []
    for entry in plan:
        if len(entry["group"]) == 1:
            continue
        height = entry["group"][0]
        low = list(range(height - 1))
        shape = (2, 1, rank, rank)
        src = space.new(*shape)
        makers, splits = [], []
        for bit in low[1:]:
            makers.append(functools.partial(space.reduce, bits=[bit], split=[bit]))
            splits.append([bit])
        makers.append(functools.partial(space.reduce, bits=low[:1]))
        steps, dst, shape = space.chain(src, shape, makers)
        makers = [functools.partial(space.gather, split=s) for s in reversed(splits)]
        more, dst, _ = space.chain(dst, shape, makers)
        sums.append((height, src, steps + more, dst))
    return sums, space


def kernel(dims, plan, tables, sums, counts, rhs_hbm, leaf_hbm, up_hbm, proj_hbm, state, last_ref, last_up, *scratch):
    bits_x, bits_y, levels, chunks, rows, rank = dims
    rhs, leaf, up, proj, rounded, coef, mix, mix_sum = scratch[:8]
    in_sems, send_sems, recv_sems, sum_send, sum_recv = scratch[8:13]
    per_chunk = counts[0]
    gx, gy = lax.axis_index("gx"), lax.axis_index("gy")
    pos = gy * (1 << bits_x) + gx

    def device(mask):
        return {"gx": gx ^ (mask & ((1 << bits_x) - 1)), "gy": gy ^ (mask >> bits_x)}

    loads = {
        "rhs": pltpu.make_async_copy(rhs_hbm, rhs, in_sems.at[0]),
        "leaf": pltpu.make_async_copy(leaf_hbm.at[0], leaf, in_sems.at[1]),
    }
    for level in range(levels):
        loads["proj", level] = pltpu.make_async_copy(proj_hbm.at[level], proj.at[level], in_sems.at[2 + 2 * level])
        if level < levels - 1:
            loads["up", level] = pltpu.make_async_copy(up_hbm.at[level], up.at[level], in_sems.at[3 + 2 * level])
    loads["last_up"] = pltpu.make_async_copy(up_hbm.at[levels - 1], last_up, in_sems.at[1 + 2 * levels])
    for load in loads.values():
        load.start()

    def need(*key):
        load = loads.pop(key if len(key) > 1 else key[0], None)
        if load is not None:
            load.wait()

    greeted = {1 << b for b in range(bits_x + bits_y)}
    for entry in plan:
        group = entry["group"]
        if len(group) == 1:
            for step in entry["reduce"] + entry["gather"]:
                greeted.update(step.masks)
        elif entry["early"]:
            greeted.update(entry["last"].masks)
        else:
            for step in entry["one"]:
                greeted.update(step.masks)
    barrier = pltpu.get_barrier_semaphore()
    for mask in sorted(greeted):
        pl.semaphore_signal(barrier, inc=1, device_id=device(mask), device_id_type=MESH)

    sent, idle = [], []

    def start(step, bufs, send, recv):
        src, dst = bufs[step.src], bufs[step.dst]
        n = step.shape[2]

        def piece(who):
            halves = pl.ds(0, step.shape[0]) if step.half is None else pl.ds((who >> step.half) & 1, 1)
            blocks = pl.ds(0, step.shape[1]) if step.block is None else pl.ds((who >> step.block) & 1, 1)
            return halves, blocks, pl.ds(pl.multiple_of(sub_index(who, step.split) * n, n), n)

        copies = []
        for k, mask in enumerate(step.masks):
            if step.kind == "gather":
                frm, to = src, dst.at[piece(pos)]
            else:
                frm, to = src.at[piece(pos ^ mask)], bufs[step.landing].at[k]
            copy = pltpu.make_async_remote_copy(
                src_ref=frm,
                dst_ref=to,
                send_sem=send(step.sem + k),
                recv_sem=recv(step.sem + k),
                device_id=device(mask),
                device_id_type=MESH,
            )
            copy.start()
            copies.append(copy)
        sent.extend(copies)
        if step.kind == "gather":
            dst[piece(pos)] = src[...]

        def finish():
            for copy in copies:
                copy.wait_recv()
            if step.kind == "reduce":
                total = src[piece(pos)]
                for k in range(len(step.masks)):
                    total = total + bufs[step.landing][k]
                dst[...] = total

        return finish

    def mixing(low, high):
        return low * levels + high

    def flow(chunk):
        lo = chunk * rows
        bufs = scratch[13 + chunk * per_chunk : 13 + (chunk + 1) * per_chunk]
        span = slice(lo, lo + rows)

        def begin(step):
            return start(step, bufs, lambda k: send_sems.at[chunk, k], lambda k: recv_sems.at[chunk, k])

        def project(height):
            need("proj", height - 1)
            table = bufs[tables[height]]
            for half in range(2):
                value = lax.dot_general(
                    rounded[span, :],
                    proj[height - 1, half * rank : (half + 1) * rank, :],
                    (((1,), (1,)), ((), ())),
                    preferred_element_type=F32,
                )
                table[half] = value.reshape(table.shape[1:])

        def keep(height, ref):
            value = ref[0].reshape(rows, rank).astype(BF16)
            if height == levels:
                last_ref[span, :] = value
            else:
                coef[height - 1, span, :] = value

        def correct(done, heights):
            for height in heights:
                delta = jnp.dot(coef[done - 1, span, :], mix[mixing(done, height)], preferred_element_type=F32)
                table = bufs[tables[height]]
                for half in range(2):
                    part = delta[:, half * rank : (half + 1) * rank]
                    table[half] = table[half] - part.reshape(table.shape[1:])

        def update(heights):
            value = state[span, :]
            for height in heights:
                need("up", height - 1)
                value = value - jnp.dot(coef[height - 1, span, :], up[height - 1], preferred_element_type=F32)
            state[span, :] = value

        need("rhs")
        need("leaf")
        value = jnp.dot(rhs[span, :], leaf[...], preferred_element_type=F32)
        state[span, :] = value
        rounded[span, :] = value.astype(BF16)
        project(1)
        if chunk == 0:
            pl.semaphore_wait(barrier, len(greeted))

        later = []
        for index, entry in enumerate(plan):
            group = entry["group"]
            after = [h for e in plan[index + 1 : index + 2] for h in e["group"]]
            beyond = [h for e in plan[index + 2 :] for h in e["group"]]
            if len(group) == 1:
                height = group[0]
                for step in entry["reduce"] + entry["gather"]:
                    finish = begin(step)
                    idle.extend(later)
                    later = []
                    yield
                    if height == 1 and step is entry["reduce"][0]:
                        for other in after:
                            project(other)
                        idle.extend(functools.partial(project, other) for other in beyond)
                    finish()
                keep(height, bufs[entry["result"]])
                if height < levels:
                    correct(height, after)
                    later = [functools.partial(correct, height, beyond), functools.partial(update, [height])]
            else:
                height = group[0]
                one, two = entry["one"], entry["two"]
                first, second = begin(one[0]), begin(two[0])
                idle.extend(later)
                later = []
                ahead = len(two) if not entry["early"] else min(len(two), len(one)) - 1
                at = 0
                for i in range(max(len(one), ahead)):
                    yield
                    if i < len(one):
                        first()
                        if i + 1 < len(one):
                            first = begin(one[i + 1])
                        else:
                            fetch = begin(entry["gather_one"][0])
                    if at < ahead:
                        second()
                        at += 1
                        if at < len(two):
                            second = begin(two[at])
                owned, joined, base = bufs[entry["owned"]], bufs[entry["joined"]], bufs[entry["partial"]]
                n = owned.shape[2]
                complete(height)
                table = mix_sum[[s[0] for s in sums].index(height)]
                delta = jnp.dot(owned[0].reshape(2 * n, rank).astype(BF16), table, preferred_element_type=F32)
                for half in range(2):
                    for block in range(2):
                        part = delta[block * n : (block + 1) * n, half * rank : (half + 1) * rank]
                        if entry["early"]:
                            joined[half, block] = -part
                        else:
                            joined[half, block] = base[half, block] - part
                finish = begin(entry["last"])
                yield
                while at < len(two):
                    second()
                    at += 1
                    if at < len(two):
                        second = begin(two[at])
                finish()
                if entry["early"]:
                    end = bufs[entry["last"].dst]
                    end[...] = end[...] + base[...]
                finish = begin(entry["gather_two"][0])
                fetch()
                for step in entry["gather_one"][1:]:
                    fetch = begin(step)
                    yield
                    fetch()
                keep(height, bufs[entry["result_one"]])
                correct(height, after)
                later = [functools.partial(correct, height, beyond)]
                if after:
                    later.append(functools.partial(correct, height + 1, beyond))
                    later.append(functools.partial(update, [height, height + 1]))
                else:
                    update([height])
                    later = []
                yield
                finish()
                for step in entry["gather_two"][1:]:
                    finish = begin(step)
                    yield
                    finish()
                keep(height + 1, bufs[entry["result_two"]])
                if after:
                    correct(height + 1, after)

    sum_bufs = scratch[13 + chunks * per_chunk :]
    running = {}

    def compute(low, high):
        need("up", low - 1)
        need("proj", high - 1)
        value = lax.dot_general(up[low - 1], proj[high - 1], (((1,), (1,)), ((), ())), preferred_element_type=F32)
        mix[mixing(low, high)] = value.astype(BF16)
        return value

    def advance(height):
        for k, (key, src, steps, dst) in enumerate(sums):
            if key != height:
                continue
            if height in running:
                at, finish = running[height]
                if finish is None:
                    return
                finish()
            else:
                at = -1
            at += 1
            if at < len(steps):
                begun = start(steps[at], sum_bufs, lambda i: sum_send.at[i], lambda i: sum_recv.at[i])
                running[height] = (at, begun)
            else:
                running[height] = (at, None)
                for half in range(2):
                    mix_sum[k, :, half * rank : (half + 1) * rank] = sum_bufs[dst][half, 0].astype(BF16)

    def complete(height):
        while running.get(height, (0, 0))[1] is not None:
            advance(height)

    def summing():
        for low in range(1, levels):
            for high in range(low + 1, levels + 1):
                value = compute(low, high)
                for height, src, _, _ in sums:
                    if (low, high) == (height, height + 1):
                        for half in range(2):
                            sum_bufs[src][half, 0] = value[:, half * rank : (half + 1) * rank]
        for height, _, _, _ in sums:
            advance(height)
        yield
        for _ in range(max([0] + [len(steps) + 1 for _, _, steps, _ in sums])):
            for height, _, _, _ in sums:
                advance(height)
            yield

    flows = [flow(chunk) for chunk in range(chunks)] + [summing()]
    while flows:
        left = []
        for item in flows:
            try:
                next(item)
                left.append(item)
            except StopIteration:
                pass
        flows = left
        while idle:
            idle.pop(0)()
    for copy in sent:
        copy.wait_send()
    for key in list(loads):
        loads.pop(key).wait()


def finish_kernel(parts, state, coef, up, out_hbm, value, sems):
    rows = state.shape[0] // parts
    copies = []
    for part in range(parts):
        span = slice(part * rows, (part + 1) * rows)
        value[span, :] = state[span, :] - jnp.dot(coef[span, :], up[...], preferred_element_type=F32)
        copy = pltpu.make_async_copy(value.at[span], out_hbm.at[span], sems.at[part])
        copy.start()
        copies.append(copy)
    for copy in copies:
        copy.wait()


def shards(rhs, leaf_inverse, up_basis, projection):
    bits_x = lax.axis_size("gx").bit_length() - 1
    bits_y = lax.axis_size("gy").bit_length() - 1
    levels, rank, points = up_basis.shape
    rows = rhs.shape[0] // CHUNKS
    plan, space, tables = build_plan(levels, bits_x, rows, rank)
    sums, more = build_sums(plan, rank)
    dims = (bits_x, bits_y, levels, CHUNKS, rows, rank)
    hbm_spec = pl.BlockSpec(memory_space=pltpu.MemorySpace.HBM)
    vmem_spec = pl.BlockSpec(memory_space=pltpu.VMEM)
    state, coefficient, last_up = pl.pallas_call(
        functools.partial(kernel, dims, plan, tables, sums, (len(space.shapes),)),
        out_shape=(
            jax.ShapeDtypeStruct((rhs.shape[0], points), F32),
            jax.ShapeDtypeStruct((rhs.shape[0], rank), BF16),
            jax.ShapeDtypeStruct((rank, points), BF16),
        ),
        in_specs=[hbm_spec] * 4,
        out_specs=(vmem_spec, vmem_spec, vmem_spec),
        scratch_shapes=[
            pltpu.VMEM(rhs.shape, BF16),
            pltpu.VMEM(leaf_inverse.shape[1:], BF16),
            pltpu.VMEM(up_basis.shape, BF16),
            pltpu.VMEM(projection.shape, BF16),
            pltpu.VMEM((rhs.shape[0], points), BF16),
            pltpu.VMEM((levels - 1, rhs.shape[0], rank), BF16),
            pltpu.VMEM((levels * (levels + 1), rank, 2 * rank), BF16),
            pltpu.VMEM((max(len(sums), 1), rank, 2 * rank), BF16),
            pltpu.SemaphoreType.DMA((2 + 2 * levels,)),
            pltpu.SemaphoreType.DMA((CHUNKS, space.sems)),
            pltpu.SemaphoreType.DMA((CHUNKS, space.sems)),
            pltpu.SemaphoreType.DMA((max(more.sems, 1),)),
            pltpu.SemaphoreType.DMA((max(more.sems, 1),)),
        ]
        + [pltpu.VMEM(shape, F32) for _ in range(CHUNKS) for shape in space.shapes]
        + [pltpu.VMEM(shape, F32) for shape in more.shapes],
        compiler_params=pltpu.CompilerParams(
            collective_id=0, has_side_effects=True, vmem_limit_bytes=44 * 2**20
        ),
    )(*[pltpu.with_memory_space_constraint(x, pltpu.MemorySpace.HBM) for x in (rhs, leaf_inverse, up_basis, projection)])
    parts = 8
    return pl.pallas_call(
        functools.partial(finish_kernel, parts),
        out_shape=jax.ShapeDtypeStruct(state.shape, F32),
        in_specs=[vmem_spec] * 3,
        out_specs=pl.BlockSpec(memory_space=pl.ANY),
        scratch_shapes=[pltpu.VMEM(state.shape, F32), pltpu.SemaphoreType.DMA((parts,))],
        compiler_params=pltpu.CompilerParams(vmem_limit_bytes=8 * 2**20),
    )(state, coefficient, last_up)


def solution(mesh):
    return jax.shard_map(
        shards,
        mesh=mesh,
        in_specs=(
            P(None, ("gy", "gx")),
            P(("gy", "gx"), None, None),
            P(None, None, ("gy", "gx")),
            P(None, None, ("gy", "gx")),
        ),
        out_specs=P(None, ("gy", "gx")),
        check_vma=False,
    )
```
